256 devices in a mesh: groups: 2 (over z), dev: 128 (over x, y, core).
Axes of the slice: x: 8, y: 8, z: 2, core: 2. Of those that a mesh axis runs over, the one named last changes fastest.
The devices are a block of a 8x8x16 slice.
Arguments:
- tokens: bfloat16 [1024, 6144], P(('groups', 'dev')), parts along dimension 0, may hold values from -6 to 6
- queries: bfloat16 [1024, 6144], P(('groups', 'dev')), parts along dimension 0, may hold values from -250 to 250
- token_kv: bfloat16 [1024, 2048], P(('groups', 'dev')), parts along dimension 0, may hold values from -6 to 6
- kv_cache: bfloat16 [1024, 64, 2048], P(('groups', 'dev')), parts along dimension 0, may hold values from -6.5 to 6.5, as said below
- context_lengths: int32 [1024], P(('groups', 'dev')), parts along dimension 0, may hold values from 2 to 64
- fresh_kv: bfloat16 [16384, 2048], P(('groups', 'dev')), parts along dimension 0, may hold values from -6 to 6
- block_counts: int32 [256], P('groups'), parts along dimension 0, may hold values from 0 to 8, as said below
- expert_ids: int32 [1024, 2], P(('groups', 'dev')), parts along dimension 0, may hold values from 0 to 3, all different within a row; in each aligned block of 4 rows (0 to 3, 4 to 7, ...) at most 3 rows name the same one
- route_weights: float32 [1024, 2], P(('groups', 'dev')), parts along dimension 0, may hold values from 0.25 to 1
- norm_gain: float32 [6144], replicated, may hold values from 0.1 to 1.9
- w_gate: bfloat16 [6144, 32768], P(None, 'dev'), may hold values from -0.078125 to 0.078125
- w_up: bfloat16 [6144, 32768], P(None, 'dev'), may hold values from -0.078125 to 0.078125
- w_down: bfloat16 [32768, 6144], P('dev'), may hold values from -0.0625 to 0.0625
Outputs:
- layer_out: bfloat16 [1024, 6144], P(('groups', 'dev')), parts along dimension 0
The draws below stay inside these ranges and needn't reach their ends.
There are 2 independent parts, one for each index of `groups`. The reference program is written for one: setup_inputs(seed, part) draws one part's arguments, and reference() takes and returns one part's arrays. A program takes and returns all parts, laid end to end along the dimension named above; an argument that names none is the same for every part. Nothing has to cross between parts.
Inputs may be any that keep to these rules, and one draw needn't show every extreme that they name: `kv_cache`: each request's cached keys and values; the table of arrays gives their range. `block_counts`: the counts sum to 512; for every device d > 0 the exclusive prefix sum before it lies between d * 4 + 1 and (d + 1) * 4; the first device takes 2 * 4 blocks. `expert_ids`: among the rows of one device no expert is named more than 3 times, and in some devices one expert is named exactly 3 times.
All inputs are finite; a program needn't handle non-finite values.
Results may differ from the reference program's by a relative error of at most 0.008.
Values may be sent and summed in bfloat16 or wider, within the bound.
A program may use at most 128 MiB of HBM per device.

```python
import math
import jax
import jax.numpy as jnp
import numpy as np
from jax import lax

D = 6144
QH = 48
KVH = 8
HD = 128
EXPERTS = 4
FF = 8192
REQ_DEV = 4
CTX = 64
BLOCK = 16
BLK_DEV = 4
MOST = 3
TOK = 512
FRESH = 8192


def cache_and_queries(key):
    base = jax.random.fold_in(key, 11)
    k_cache = jax.random.fold_in(base, 0)
    k_query = jax.random.fold_in(base, 2)
    width = 2 * KVH * HD
    cache = jnp.clip(jax.random.normal(k_cache, (TOK, CTX, width), jnp.float32), -6.0, 6.0)
    queries = jax.random.normal(k_query, (TOK, QH * HD), jnp.float32)
    queries = jnp.clip(queries, -250.0, 250.0)
    return (cache, queries)


def draw_kv_cache(key, part):
    cache, queries = cache_and_queries(key)
    return cache.astype(jnp.bfloat16)


def draw_queries(key, part):
    cache, queries = cache_and_queries(key)
    return queries.astype(jnp.bfloat16)


def draw_block_counts(key, part):
    devices = TOK // REQ_DEV
    carried = jax.random.randint(jax.random.fold_in(key, 23), (devices,), 1, BLK_DEV + 1)
    places = jnp.arange(devices, dtype=jnp.int32)
    carried = jnp.where(places == 0, BLK_DEV, carried)
    carried = jnp.where(places == devices - 1, 0, carried)
    before = jnp.concatenate([jnp.zeros((1,), jnp.int32), carried[:-1]], 0)
    return (BLK_DEV + carried - before).astype(jnp.int32)


def plant(values, stream_key, low, high):
    place = [jax.random.randint(jax.random.fold_in(stream_key, axis), (), 0, length) for axis, length in enumerate(values.shape)]
    widest = values.shape.index(max(values.shape))
    neighbour = place[:widest] + [(place[widest] + 1) % values.shape[widest]] + place[widest + 1:]
    return values.at[tuple(place)].set(low).at[tuple(neighbour)].set(high)


def steps_of(key, shape, cuts, least, largest):
    loudness, own = 1.0, jax.random.fold_in(key, 6)
    for dim, parts in cuts:
        draws = jnp.exp(jax.random.uniform(jax.random.fold_in(own, dim), (parts,), jnp.float32, least / len(cuts), largest / len(cuts)))
        loudness = loudness * jnp.repeat(draws, shape[dim] // parts).reshape([-1 if axis == dim else 1 for axis in range(len(shape))])
    return loudness


def deal_out(key, own, number, rows, number_of, top, most, skew):
    sequence = jax.random.permutation(key, number_of)
    packed, common = load_shares(number_of, rows * top, most, skew, True), load_shares(number_of, rows * top, most, skew, False)
    places = jnp.arange(number_of)

    def named(lengths, rotation):
        used = int((lengths > 0).sum())
        fixed = max(1, used // 4)
        passed = fixed + (places - fixed + rotation * (used - fixed)) % max(1, number_of - fixed)
        return jnp.zeros((number_of,), jnp.int32).at[sequence[jnp.where(places < fixed, places, passed)]].set(jnp.asarray(lengths, jnp.int32))

    lengths = jnp.where(number % 4 == 0, named(packed, number // 4), named(common, number - number // 4 - 1))
    mixed = jax.random.permutation(jax.random.fold_in(own, 3), number_of)
    source_of, taker = mixed[0:number_of // 2 * 2:2], mixed[1:number_of // 2 * 2:2]
    slack = jnp.minimum(lengths[source_of] - 1, most - lengths[taker]) // 2
    slack = jnp.where((source_of == sequence[0]) | (taker == sequence[0]) | (lengths[taker] == 0), 0, jnp.maximum(slack, 0))
    passed = jax.random.randint(jax.random.fold_in(own, 4), (number_of // 2,), 0, 1 << 20) % (slack + 1)
    lengths = lengths.at[source_of].add(-passed).at[taker].add(passed)
    members = jnp.searchsorted(jnp.cumsum(lengths), jnp.arange(rows * top), side="right").astype(jnp.int32)
    table = members.reshape(top, rows).T
    table = table[jax.random.permutation(jax.random.fold_in(own, 1), rows)]
    rotation = jax.random.randint(jax.random.fold_in(own, 2), (rows, 1), 0, top)
    return jnp.take_along_axis(table, (jnp.arange(top)[None, :] + rotation) % top, axis=1)


def load_shares(amount, total, bound, lean, full):
    portions = [(1 << 20) // math.isqrt(rank ** lean) + 1 for rank in range(1, amount + 1)]
    largest = bound if full else min(bound, max(-(-total // amount), total * portions[0] // sum(portions)))
    least = 1 if total - largest >= amount - 1 else 0
    counts, rest = [largest] + [least] * (amount - 1), total - largest - least * (amount - 1)
    while rest > 0:
        free = [i for i in range(1, amount) if counts[i] < largest] or [i for i in range(1, amount) if counts[i] < bound]
        pool, left = sum([portions[i] for i in free]), rest
        for i in free:
            addition = min(bound - counts[i], max(1, left * portions[i] // pool), rest)
            counts[i] = counts[i] + addition
            rest = rest - addition
    return np.array(counts)


def bell_draw(rng, shape, scale, reach, cuts=(), held_as=jnp.bfloat16):
    loudness = steps_of(rng, shape, cuts, -0.22, 0.18) if cuts else 1.0
    drawn = jax.random.normal(rng, shape, jnp.float32) * scale * loudness
    return jnp.minimum(jnp.maximum(drawn, -reach), reach).astype(held_as)


def setup_inputs(seed: int = 0, part: int = 0) -> dict:
    splits = jax.random.split(jax.random.key(seed), 14)
    part_splits = jax.random.split(jax.random.fold_in(splits[13], part), 14)
    tokens = bell_draw(part_splits[0], (TOK, D), 1.0, 6.0, ((0, 128),))
    queries = draw_queries(jax.random.fold_in(jax.random.fold_in(splits[13], part), 71), part)
    token_kv = bell_draw(part_splits[2], (TOK, 2 * KVH * HD), 1.0, 6.0, ((0, 128),))
    kv_cache = draw_kv_cache(jax.random.fold_in(jax.random.fold_in(splits[13], part), 71), part)
    context_lengths = plant(jax.random.randint(part_splits[4], (TOK,), 2, CTX + 1), jax.random.fold_in(part_splits[4], 1), 2, CTX).astype(jnp.int32)
    fresh_kv = bell_draw(part_splits[5], (FRESH, 2 * KVH * HD), 1.0, 6.0, ((0, 128),))
    block_counts = draw_block_counts(jax.random.fold_in(jax.random.fold_in(splits[13], part), 71), part)
    expert_ids_keys = jax.random.split(jax.random.fold_in(part_splits[7], 1), TOK // REQ_DEV)
    expert_ids_turns = jax.random.permutation(jax.random.fold_in(part_splits[7], 3), TOK // REQ_DEV)
    expert_ids = jax.vmap(lambda own, number: deal_out(jax.random.fold_in(part_splits[7], 2), own, number, REQ_DEV, EXPERTS, 2, MOST, 2))(expert_ids_keys, expert_ids_turns).reshape((TOK, 2))
    route_weights = jnp.clip(jnp.exp(math.log(1.0) - 1.3862944 * jax.random.uniform(part_splits[8], (TOK, 2), jnp.float32) ** steps_of(part_splits[8], (TOK, 2), ((0, 128),), -0.2, 0.2)), 0.25, 1.0)
    norm_gain = jnp.clip(1.0 + 0.18 * jax.random.normal(splits[9], (D,), jnp.float32), 0.1, 1.9)
    w_gate = bell_draw(splits[10], (D, EXPERTS * FF), D ** -0.5, 0.078125, ((1, 128),))
    w_up = bell_draw(splits[11], (D, EXPERTS * FF), D ** -0.5, 0.078125, ((1, 128),))
    w_down = bell_draw(splits[12], (EXPERTS * FF, D), FF ** -0.5, 0.0625, ((0, 128),))
    return {"tokens": tokens, "queries": queries, "token_kv": token_kv, "kv_cache": kv_cache, "context_lengths": context_lengths, "fresh_kv": fresh_kv, "block_counts": block_counts, "expert_ids": expert_ids, "route_weights": route_weights, "norm_gain": norm_gain, "w_gate": w_gate, "w_up": w_up, "w_down": w_down}


EPS = 1e-05
NEG = -1e+30

def attend(query, cache, lens, own, window, first, last):
    reqs = query.shape[0]
    length = cache.shape[1]
    group = QH // KVH
    half = KVH * HD
    scale = 1.0 / math.sqrt(HD)
    q_all = query.astype(jnp.float32).reshape(reqs, KVH, group, HD)
    keys_c = cache[:, :, :half].astype(jnp.float32).reshape(reqs, length, KVH, HD)
    vals_c = cache[:, :, half:].astype(jnp.float32).reshape(reqs, length, KVH, HD)
    keys_w = window[:, :half].astype(jnp.float32).reshape(-1, KVH, HD)
    vals_w = window[:, half:].astype(jnp.float32).reshape(-1, KVH, HD)
    keys_o = own[:, :half].astype(jnp.float32).reshape(reqs, KVH, HD)
    vals_o = own[:, half:].astype(jnp.float32).reshape(reqs, KVH, HD)
    s_cache = jnp.einsum('rkgh,rpkh->rkgp', q_all, keys_c) * scale
    places = jnp.arange(length, dtype=jnp.int32)
    s_cache = jnp.where(places[None, None, None, :] < lens[:, None, None, None], s_cache, NEG)
    s_win = jnp.einsum('rkgh,pkh->rkgp', q_all, keys_w) * scale
    rows = jnp.arange(window.shape[0], dtype=jnp.int32)
    live = (rows >= first) & (rows < last)
    leader = jnp.arange(reqs, dtype=jnp.int32) == 0
    usable = leader[:, None] & live[None, :]
    s_win = jnp.where(usable[:, None, None, :], s_win, NEG)
    s_own = jnp.einsum('rkgh,rkh->rkg', q_all, keys_o) * scale
    top = jnp.maximum(jnp.maximum(lax.optimization_barrier(jnp.max(s_cache, -1)), lax.optimization_barrier(jnp.max(s_win, -1))), s_own)
    e_cache = jnp.exp(s_cache - top[..., None])
    e_win = jnp.exp(s_win - top[..., None])
    e_own = jnp.exp(s_own - top)
    total = lax.optimization_barrier(jnp.sum(e_cache, -1)) + lax.optimization_barrier(jnp.sum(e_win, -1)) + e_own
    p_cache = (e_cache / total[..., None]).astype(jnp.bfloat16).astype(jnp.float32)
    p_win = (e_win / total[..., None]).astype(jnp.bfloat16).astype(jnp.float32)
    p_own = (e_own / total).astype(jnp.bfloat16).astype(jnp.float32)
    mixed = jnp.einsum('rkgp,rpkh->rkgh', p_cache, vals_c)
    mixed = mixed + jnp.einsum('rkgp,pkh->rkgh', p_win, vals_w)
    mixed = mixed + p_own[..., None] * vals_o[:, :, None, :]
    return mixed.reshape(reqs, QH * HD)

def reference(tokens, queries, token_kv, kv_cache, context_lengths, fresh_kv, block_counts, expert_ids, route_weights, norm_gain, w_gate, w_up, w_down):
    devices = TOK // REQ_DEV
    width = 2 * KVH * HD
    span = BLK_DEV * BLOCK
    fresh = fresh_kv.reshape(devices, span, width)
    following = jnp.concatenate([fresh[1:], jnp.zeros((1, span, width), fresh.dtype)], 0)
    windows = jnp.concatenate([fresh, following], 1)
    offsets = jnp.cumsum(block_counts) - block_counts
    starts = (offsets - jnp.arange(devices, dtype=jnp.int32) * BLK_DEV).astype(jnp.int32)
    ends = (starts + block_counts).astype(jnp.int32)

    def one_device(pieces):
        q_dev, c_dev, l_dev, o_dev, w_dev, s_dev, e_dev = pieces
        return attend(q_dev, c_dev, l_dev, o_dev, w_dev, s_dev * BLOCK, e_dev * BLOCK)
    attn = lax.map(one_device, (queries.reshape(devices, REQ_DEV, QH * HD), kv_cache.reshape(devices, REQ_DEV, CTX, width), context_lengths.reshape(devices, REQ_DEV), token_kv.reshape(devices, REQ_DEV, width), windows, starts, ends)).reshape(TOK, D)
    hidden_state = tokens.astype(jnp.float32) + attn
    spread = lax.optimization_barrier(jnp.mean(hidden_state * hidden_state, -1, keepdims=True))
    normed = (hidden_state * lax.rsqrt(spread + EPS) * norm_gain).astype(jnp.bfloat16)
    labels = jnp.arange(EXPERTS, dtype=jnp.int32)
    coef = lax.optimization_barrier(jnp.sum(route_weights[:, :, None] * (expert_ids[:, :, None] == labels[None, None, :]).astype(jnp.float32), 1))
    shards = devices // EXPERTS
    units = FF // shards
    gates = w_gate.reshape(D, EXPERTS, FF).transpose(1, 0, 2)
    ups = w_up.reshape(D, EXPERTS, FF).transpose(1, 0, 2)
    downs = w_down.reshape(EXPERTS, shards, units, D)

    def one_expert(pieces):
        gate_e, up_e, down_e, coef_e = pieces
        gate_v = jnp.dot(normed, gate_e, preferred_element_type=jnp.float32)
        up_v = jnp.dot(normed, up_e, preferred_element_type=jnp.float32)
        act = (jax.nn.silu(gate_v) * up_v).astype(jnp.bfloat16)
        act_parts = act.reshape(TOK, shards, units).transpose(1, 0, 2)

        def add_shard(total, piece):
            act_s, down_s = piece
            part = jnp.dot(act_s, down_s, preferred_element_type=jnp.float32).astype(jnp.bfloat16)
            part = lax.optimization_barrier(part)
            return (total + part.astype(jnp.float32), None)
        summed, unused = lax.scan(add_shard, jnp.zeros((TOK, D), jnp.float32), (act_parts, down_e))
        return coef_e[:, None] * summed
    contrib = lax.map(one_expert, (gates, ups, downs, coef.T))
    moe = lax.optimization_barrier(jnp.sum(contrib, 0))
    return (hidden_state + moe).astype(jnp.bfloat16)
```

```python
import math

import jax
import jax.numpy as jnp
from jax import lax
from jax.sharding import Mesh
from jax.sharding import PartitionSpec as P
from jax.experimental import pallas as pl
from jax.experimental.pallas import tpu as pltpu

QH = 48
KVH = 8
HD = 128
EXPERTS = 4
BLOCK = 16
DEV = ("dev_0", "dev_1", "dev_2")
GROUPS_DEV = ("groups", "dev_0", "dev_1", "dev_2")


EPS = 1e-05
NEG = -1e30


def passed_along(value, axis, steps):
    count = lax.axis_size(axis)
    leading, last = (max(0, -steps), min(count, count - steps))
    return lax.ppermute(value, axis, [(source, source + steps) for source in range(leading, last)])


MESH_ID = pl.DeviceIdType.MESH
RING = ("dev_1", "dev_0")
LINE = ("dev_0", "dev_1")
SUBS = 2


def exchange_kernel(
    rows_ref, coef_ref, perm_ref, back_ref, gate_hbm, up_hbm, down_hbm, out_ref,
    gathered, coefs, wide, act, part, crossed, hops, fin, w_gate, w_up, w_down,
    sem_w, c_send, c_recv, g1_send, g1_recv, g2_send, g2_recv, gx_send, gx_recv,
    x_send, x_recv, r_send, r_recv, f_send, f_recv,
):
    n = lax.axis_size("dev_0")
    half_n = n // 2
    core = lax.axis_index("dev_2")
    other = 1 - core
    sgn = 1 - 2 * core
    xy = {"dev_0": lax.axis_index("dev_0"), "dev_1": lax.axis_index("dev_1")}
    pos = [xy[a] for a in RING]
    line = [xy[a] for a in LINE]
    width = rows_ref.shape[2]
    per = n // SUBS

    def wrap(v):
        return lax.rem(v + 2 * n, n)

    loads = [
        pltpu.make_async_copy(src, dst, sem_w.at[i])
        for i, (src, dst) in enumerate(((gate_hbm, w_gate), (up_hbm, w_up), (down_hbm, w_down)))
    ]
    for load in loads:
        load.start()

    barrier = pltpu.get_barrier_semaphore()
    pl.semaphore_signal(barrier, inc=1, device_id={"dev_2": other}, device_id_type=MESH_ID)
    for axis in LINE:
        for j in range(1, n):
            pl.semaphore_signal(
                barrier, inc=1, device_id={axis: wrap(xy[axis] + j)}, device_id_type=MESH_ID
            )
    pl.semaphore_wait(barrier, 2 * (n - 1) + 1)

    pending = []

    def send(src, dst, s_sem, r_sem, where):
        copy = pltpu.make_async_remote_copy(
            src_ref=src, dst_ref=dst, send_sem=s_sem, recv_sem=r_sem,
            device_id=where, device_id_type=MESH_ID,
        )
        copy.start()
        pending.append(copy)
        return copy

    gathered[0, core, pos[0], line[0]] = rows_ref[0]
    gathered[1, core, pos[1], line[1]] = rows_ref[1]
    coefs[core, xy["dev_1"], xy["dev_0"]] = coef_ref[0]
    firsts = []
    for j in range(1, n):
        firsts.append(
            send(
                coef_ref.at[0], coefs.at[core, xy["dev_1"], xy["dev_0"]], c_send.at[j], c_recv.at[j],
                {"dev_0": wrap(xy["dev_0"] + j)},
            )
        )
        for h in range(2):
            firsts.append(
                send(
                    rows_ref.at[h], gathered.at[h, core, pos[h], line[h]],
                    g1_send.at[h, j], g1_recv.at[h, j], {LINE[h]: wrap(line[h] + j)},
                )
            )
    for copy in firsts:
        copy.wait_recv()
    seconds = []
    for j in range(1, n):
        seconds.append(
            send(
                coefs.at[core, xy["dev_1"]], coefs.at[core, xy["dev_1"]],
                c_send.at[n + j], c_recv.at[n + j], {"dev_1": wrap(xy["dev_1"] + j)},
            )
        )

    crossing = []

    def cross(h, where, sub, slot):
        ref = gathered.at[h, core, where, pl.ds(sub * per, per)]
        crossing.append(
            send(ref, ref, gx_send.at[h, slot, sub], gx_recv.at[h, slot, sub], {"dev_2": other})
        )

    last = {}
    for s in range(1, half_n + 1):
        for sub in range(SUBS):
            for h in range(2):
                for way, hops_of in ((0, half_n), (1, half_n - 1)):
                    if s > hops_of:
                        continue
                    turn = sgn if way == 0 else -sgn
                    where = wrap(pos[h] - turn * (s - 1))
                    if s > 1:
                        last[h, way, sub].wait_recv()
                    ref = gathered.at[h, core, where, pl.ds(sub * per, per)]
                    last[h, way, sub] = send(
                        ref, ref, g2_send.at[h, way, s - 1, sub], g2_recv.at[h, way, s - 1, sub],
                        {RING[h]: wrap(pos[h] + turn)},
                    )
                    if s > 1:
                        cross(h, where, sub, way * half_n + s - 1)
                    elif way == 0:
                        cross(h, where, sub, 0)
    for sub in range(SUBS):
        for h in range(2):
            for way, hops_of in ((0, half_n), (1, half_n - 1)):
                turn = sgn if way == 0 else -sgn
                last[h, way, sub].wait_recv()
                cross(h, wrap(pos[h] - turn * hops_of), sub, way * half_n + hops_of)
    for copy in seconds:
        copy.wait_recv()
    both = send(coefs.at[core], coefs.at[core], c_send.at[0], c_recv.at[0], {"dev_2": other})
    both.wait_recv()
    for copy in crossing:
        copy.wait_recv()
    for load in loads:
        load.wait()

    expert = (xy["dev_0"] * (2 * n) + xy["dev_1"] * 2 + core) // (2 * n * n // EXPERTS)
    toks = 4
    batch = 2 * n * toks
    batches = n // 2
    tile = 256

    def spread(i, carry):
        cc = jnp.where(i < batches, other, core)
        yp = lax.rem(i, batches) * 2
        for t in range(width // tile):
            cols = pl.ds(t * tile, tile)
            for h in range(2):
                if h == 0:
                    z = gathered[0, cc, pl.ds(yp, 2), :, :, cols].reshape(4 * batch, tile)
                else:
                    z = jnp.concatenate(
                        [
                            gathered[1, cc, :, yp + k, :, cols].reshape(2 * batch, tile)
                            for k in range(2)
                        ],
                        0,
                    )
                z = jnp.dot(perm_ref[...], z, preferred_element_type=jnp.float32).astype(jnp.bfloat16)
                for q in range(4):
                    wide[pl.ds(i * batch, batch), pl.ds((2 * q + h) * width + t * tile, tile)] = z[
                        q * batch : (q + 1) * batch
                    ]
        return carry

    lax.fori_loop(0, 2 * batches, spread, 0)

    def experts(i, carry):
        at = pl.ds(i * 4 * batch, 4 * batch)
        cc = jnp.where(i < 1, other, core)
        gate = jnp.dot(wide[at], w_gate[...], preferred_element_type=jnp.float32)
        up = jnp.dot(wide[at], w_up[...], preferred_element_type=jnp.float32)
        sub8 = lax.broadcasted_iota(jnp.int32, (8, 128), 0)
        lane8 = lax.broadcasted_iota(jnp.int32, (8, 128), 1)
        keep = lane8 == lax.rem(sub8, toks) * EXPERTS + expert
        pieces = []
        for y in range(n):
            for x in range(0, n, 2):
                both = jnp.where(sub8 < toks, coefs[cc, y, x], coefs[cc, y, x + 1])
                pieces.append(jnp.sum(jnp.where(keep, both, 0.0), 1, keepdims=True))
        coef = jnp.concatenate(pieces, 0)
        act[at] = (gate / (1.0 + jnp.exp(-gate)) * up * coef).astype(jnp.bfloat16)
        return carry

    lax.fori_loop(0, 2, experts, 0)

    crossed_copies = []
    for turn in range(2):
        cc = other if turn == 0 else core
        at = pl.ds(turn * 4 * batch, 4 * batch)

        def down(t, carry):
            cols = pl.ds(pl.multiple_of(t * tile, tile), tile)
            wide[at, cols] = jnp.dot(
                act[at], w_down[:, cols], preferred_element_type=jnp.float32
            ).astype(jnp.bfloat16)
            return carry

        lax.fori_loop(0, wide.shape[1] // tile, down, 0)

        def gathered_back(i, carry):
            rows = pl.ds((turn * batches + i) * batch, batch)
            yp = 2 * i
            for t in range(width // tile):
                cols = pl.ds(t * tile, tile)
                for h in range(2):
                    z = jnp.concatenate(
                        [
                            wide[rows, pl.ds((2 * q + h) * width + t * tile, tile)]
                            for q in range(4)
                        ],
                        0,
                    )
                    z = jnp.dot(back_ref[...], z, preferred_element_type=jnp.float32)
                    z = z.astype(jnp.bfloat16).reshape(2, n, 16, tile)
                    if h == 0:
                        part[0, cc, pl.ds(yp, 2), :, :, cols] = z
                    else:
                        for k in range(2):
                            part[1, cc, :, yp + k, :, cols] = z[k]
            return carry

        lax.fori_loop(0, batches, gathered_back, 0)
        if turn == 0:
            for h in range(2):
                for k in range(batches):
                    at_k = pl.ds(2 * k, 2)
                    crossed_copies.append(
                        send(
                            part.at[h, other, at_k], crossed.at[h, at_k],
                            x_send.at[h, k], x_recv.at[h, k], {"dev_2": other},
                        )
                    )
    for copy in crossed_copies:
        copy.wait_recv()

    held = {}
    for s in range(1, half_n + 1):
        for sub in range(SUBS):
            for h in range(2):
                for way, hops_of in ((0, half_n), (1, half_n - 1)):
                    if s > hops_of:
                        continue
                    turn = sgn if way == 0 else -sgn
                    dest = wrap(pos[h] + turn * (hops_of + 1 - s))
                    at = pl.ds(sub * per, per)
                    total = part[h, core, dest, at].astype(jnp.float32) + crossed[
                        h, dest, at
                    ].astype(jnp.float32)
                    if s > 1:
                        held[h, way, sub].wait_recv()
                        total = total + hops[h, way, s - 2, at].astype(jnp.float32)
                    part[h, core, dest, at] = total.astype(jnp.bfloat16)
                    held[h, way, sub] = send(
                        part.at[h, core, dest, at], hops.at[h, way, s - 1, at],
                        r_send.at[h, way, s - 1, sub], r_recv.at[h, way, s - 1, sub],
                        {RING[h]: wrap(pos[h] + turn)},
                    )
    finals = []
    for sub in range(SUBS):
        for h in range(2):
            at = pl.ds(sub * per, per)
            total = part[h, core, pos[h], at].astype(jnp.float32) + crossed[h, pos[h], at].astype(
                jnp.float32
            )
            for way, hops_of in ((0, half_n), (1, half_n - 1)):
                held[h, way, sub].wait_recv()
                total = total + hops[h, way, hops_of - 1, at].astype(jnp.float32)
            part[h, core, pos[h], at] = total.astype(jnp.bfloat16)
    for j in range(1, n):
        for h in range(2):
            finals.append(
                send(
                    part.at[h, core, pos[h], wrap(line[h] + j)], fin.at[h, j],
                    f_send.at[h, j], f_recv.at[h, j], {LINE[h]: wrap(line[h] + j)},
                )
            )
    for copy in finals:
        copy.wait_recv()
    for h in range(2):
        total = part[h, core, pos[h], line[h]].astype(jnp.float32)
        for j in range(1, n):
            total = total + fin[h, j].astype(jnp.float32)
        out_ref[h] = total
    for copy in pending:
        copy.wait_send()


def exchange(rows, coef, w_gate, w_up, w_down):
    n = lax.axis_size("dev_0")
    width = rows.shape[2]
    full = w_gate.shape[0]
    units = w_gate.shape[1]
    tokens = 2 * n * n * 4
    size = 4 * 2 * n * 4
    r = jnp.arange(size, dtype=jnp.int32)
    q, b, t = r // (size // 4), (r // 4) % (size // 16), r % 4
    source = b * 16 + q * 4 + t
    perm = (source[:, None] == r[None, :]).astype(jnp.bfloat16)
    back = perm.T
    vmem = pl.BlockSpec(memory_space=pltpu.VMEM)
    anyspace = pl.BlockSpec(memory_space=pl.ANY)
    bf = jnp.bfloat16
    dma = pltpu.SemaphoreType.DMA
    half_n = n // 2
    return pl.pallas_call(
        exchange_kernel,
        out_shape=jax.ShapeDtypeStruct(rows.shape, jnp.float32),
        in_specs=[vmem] * 4 + [anyspace] * 3,
        out_specs=vmem,
        scratch_shapes=[
            pltpu.VMEM((2, 2, n, n, 16, width), bf),
            pltpu.VMEM((2, n, n, 1, 128), jnp.float32),
            pltpu.VMEM((tokens, full), bf),
            pltpu.VMEM((tokens, units), bf),
            pltpu.VMEM((2, 2, n, n, 16, width), bf),
            pltpu.VMEM((2, n, n, 16, width), bf),
            pltpu.VMEM((2, 2, half_n, n, 16, width), bf),
            pltpu.VMEM((2, n, 16, width), bf),
            pltpu.VMEM(w_gate.shape, bf),
            pltpu.VMEM(w_up.shape, bf),
            pltpu.VMEM(w_down.shape, bf),
            dma((3,)),
            dma((2 * n,)), dma((2 * n,)),
            dma((2, n)), dma((2, n)),
            dma((2, 2, half_n, SUBS)), dma((2, 2, half_n, SUBS)),
            dma((2, 2 * half_n, SUBS)), dma((2, 2 * half_n, SUBS)),
            dma((2, n // 2)), dma((2, n // 2)),
            dma((2, 2, half_n, SUBS)), dma((2, 2, half_n, SUBS)),
            dma((2, n)), dma((2, n)),
        ],
        compiler_params=pltpu.CompilerParams(
            collective_id=0, has_side_effects=True, vmem_limit_bytes=58 * 1024 * 1024
        ),
    )(rows, coef, perm, back, w_gate, w_up, w_down)


def attend(query, cache, lens, own, window, first, last):
    reqs = query.shape[0]
    length = cache.shape[1]
    group = QH // KVH
    half = KVH * HD
    scale = 1.0 / math.sqrt(HD)
    q_all = query.reshape(reqs, KVH, group, HD)
    keys_c = cache[:, :, :half].reshape(reqs, length, KVH, HD)
    vals_c = cache[:, :, half:].reshape(reqs, length, KVH, HD)
    keys_w = window[:, :half].reshape(-1, KVH, HD)
    vals_w = window[:, half:].reshape(-1, KVH, HD)
    keys_o = own[:, :half].reshape(reqs, KVH, HD)
    vals_o = own[:, half:].astype(jnp.float32).reshape(reqs, KVH, HD)
    s_cache = (
        jnp.einsum("rkgh,rpkh->rkgp", q_all, keys_c, preferred_element_type=jnp.float32) * scale
    )
    places = jnp.arange(length, dtype=jnp.int32)
    s_cache = jnp.where(places[None, None, None, :] < lens[:, None, None, None], s_cache, NEG)
    s_win = jnp.einsum("rkgh,pkh->rkgp", q_all, keys_w, preferred_element_type=jnp.float32) * scale
    rows = jnp.arange(window.shape[0], dtype=jnp.int32)
    live = (rows >= first) & (rows < last)
    leader = jnp.arange(reqs, dtype=jnp.int32) == 0
    usable = leader[:, None] & live[None, :]
    s_win = jnp.where(usable[:, None, None, :], s_win, NEG)
    s_own = jnp.einsum("rkgh,rkh->rkg", q_all, keys_o, preferred_element_type=jnp.float32) * scale
    top = jnp.maximum(jnp.maximum(jnp.max(s_cache, -1), jnp.max(s_win, -1)), s_own)
    e_cache = jnp.exp(s_cache - top[..., None])
    e_win = jnp.exp(s_win - top[..., None])
    e_own = jnp.exp(s_own - top)
    total = jnp.sum(e_cache, -1) + jnp.sum(e_win, -1) + e_own
    p_cache = (e_cache / total[..., None]).astype(jnp.bfloat16)
    p_win = (e_win / total[..., None]).astype(jnp.bfloat16)
    p_own = (e_own / total).astype(jnp.bfloat16).astype(jnp.float32)
    mixed = jnp.einsum("rkgp,rpkh->rkgh", p_cache, vals_c, preferred_element_type=jnp.float32)
    mixed = mixed + jnp.einsum("rkgp,pkh->rkgh", p_win, vals_w, preferred_element_type=jnp.float32)
    mixed = mixed + p_own[..., None] * vals_o[:, :, None, :]
    return mixed.reshape(reqs, QH * HD)


def per_device(
    tokens,
    queries,
    token_kv,
    kv_cache,
    context_lengths,
    fresh_kv,
    block_counts,
    expert_ids,
    route_weights,
    norm_gain,
    w_gate,
    w_up,
    w_down,
):
    me = lax.axis_index(DEV)
    reqs = tokens.shape[0]
    width = tokens.shape[1]
    span = fresh_kv.shape[0]
    following = passed_along(fresh_kv, DEV, -1)
    window = jnp.concatenate([fresh_kv, following], 0)
    offsets = jnp.cumsum(block_counts) - block_counts
    mine = lax.dynamic_index_in_dim(offsets, me, 0, keepdims=False)
    taken = lax.dynamic_index_in_dim(block_counts, me, 0, keepdims=False)
    first = (mine - me * (span // BLOCK)) * BLOCK
    last = first + taken * BLOCK
    attn = attend(queries, kv_cache, context_lengths, token_kv, window, first, last)
    hidden_state = tokens.astype(jnp.float32) + attn
    spread = jnp.mean(hidden_state * hidden_state, -1, keepdims=True)
    normed = (hidden_state * lax.rsqrt(spread + EPS) * norm_gain).astype(jnp.bfloat16)
    labels = jnp.arange(EXPERTS, dtype=jnp.int32)
    coef = jnp.sum(
        route_weights[:, :, None] * (expert_ids[:, :, None] == labels).astype(jnp.float32), 1
    ).reshape(1, 1, reqs * EXPERTS)
    coef = jnp.pad(coef, ((0, 0), (0, 0), (0, 128 - reqs * EXPERTS)))
    stacked = normed.reshape(reqs, 4, 2, width // 8).transpose(2, 1, 0, 3).reshape(2, 4 * reqs, width // 8)
    moe = exchange(stacked, coef, w_gate, w_up, w_down)
    moe = moe.reshape(2, 4, reqs, width // 8).transpose(2, 1, 0, 3).reshape(reqs, width)
    return (hidden_state + moe).astype(jnp.bfloat16)


def solution(mesh):
    split = Mesh(
        mesh.devices.reshape(mesh.shape["groups"], 8, 8, 2), ("groups", "dev_0", "dev_1", "dev_2")
    )
    return jax.shard_map(
        per_device,
        mesh=split,
        in_specs=(
            P(GROUPS_DEV, None),
            P(GROUPS_DEV, None),
            P(GROUPS_DEV, None),
            P(GROUPS_DEV, None, None),
            P(GROUPS_DEV),
            P(GROUPS_DEV, None),
            P("groups"),
            P(GROUPS_DEV, None),
            P(GROUPS_DEV, None),
            P(),
            P(None, DEV),
            P(None, DEV),
            P(DEV, None),
        ),
        out_specs=P(GROUPS_DEV, None),
        check_vma=False,
    )
```

```python
import math

import jax
import jax.numpy as jnp
from jax import lax
from jax.sharding import Mesh
from jax.sharding import PartitionSpec as P
from jax.experimental import pallas as pl
from jax.experimental.pallas import tpu as pltpu

QH = 48
KVH = 8
HD = 128
EXPERTS = 4
BLOCK = 16
DEV = ("dev_0", "dev_1", "dev_2")
GROUPS_DEV = ("groups", "dev_0", "dev_1", "dev_2")


EPS = 1e-05
NEG = -1e30


MESH_ID = pl.DeviceIdType.MESH
RING = ("dev_1", "dev_0")
LINE = ("dev_0", "dev_1")
OFFSETS = (0, 1, -1, 2, -2, 3, -3, 4)
GROUPS_OF_BLOCKS = ((0, 3), (3, 2), (5, 3))


def slot_at(sign, distance):
    if distance in (0, 4):
        return 2 * distance - distance // 4
    return 2 * distance - (1 + sign) // 2


def slots_of(distance):
    if distance == 0:
        return (0, 1)
    return (2 * distance - 1, 1 if distance == 4 else 2)


def attend(lens_ref, counts_ref, query8, kv_all, me, reqs, span, length):
    sub8 = lax.broadcasted_iota(jnp.int32, (8, HD), 0)
    tiles = []
    for h in range(0, QH, 2):
        a = query8[:, h * HD : (h + 1) * HD]
        b = query8[:, (h + 1) * HD : (h + 2) * HD]
        tiles.append(jnp.where(sub8 < reqs, a, b))
    group = QH // KVH
    rows = group * reqs
    total_keys = kv_all.shape[0]
    half = KVH * HD
    counts = counts_ref[...]
    lane = lax.broadcasted_iota(jnp.int32, counts.shape, 1)
    offset = jnp.sum(jnp.where(lane < me, counts, 0), 1, keepdims=True)
    taken = jnp.sum(jnp.where(lane == me, counts, 0), 1, keepdims=True)
    first = offset * BLOCK - me * span
    stop = first + taken * BLOCK
    key = lax.broadcasted_iota(jnp.int32, (1, total_keys), 1)
    cached = reqs * length
    owner = jnp.full((1, total_keys), -1, jnp.int32)
    for t in range(reqs):
        place = key - t * length
        mine = (place >= 0) & (place < length) & (place < lens_ref[t])
        owner = jnp.where(mine, t, owner)
    place = key - cached
    live = (place >= 0) & (place < 2 * span) & (place >= first) & (place < stop)
    owner = jnp.where(live, 0, owner)
    place = key - (cached + 2 * span)
    owner = jnp.where((place >= 0) & (place < reqs), place, owner)
    row = lax.rem(lax.broadcasted_iota(jnp.int32, (rows, total_keys), 0), reqs)
    valid = row == owner
    mixed = []
    for k in range(KVH):
        q = jnp.concatenate(tiles[k * group // 2 : (k + 1) * group // 2], 0).astype(jnp.bfloat16)
        s = lax.dot_general(
            q,
            kv_all[:, k * HD : (k + 1) * HD],
            (((1,), (1,)), ((), ())),
            preferred_element_type=jnp.float32,
        ) * (1.0 / math.sqrt(HD))
        s = jnp.where(valid, s, NEG)
        e = jnp.exp(s - jnp.max(s, 1, keepdims=True))
        p = (e / jnp.sum(e, 1, keepdims=True)).astype(jnp.bfloat16)
        mixed.append(
            jnp.dot(
                p,
                kv_all[:, half + k * HD : half + (k + 1) * HD],
                preferred_element_type=jnp.float32,
            )
        )
    parts = []
    for k in range(KVH):
        for i in range(group // 2):
            piece = mixed[k][8 * i : 8 * i + 8]
            turned = pltpu.roll(piece, reqs, 0)
            parts.append(jnp.where(sub8 < reqs, piece, turned))
            parts.append(jnp.where(sub8 < reqs, turned, piece))
    return jnp.concatenate(parts, 1)


def layer_kernel(
    lens_ref, ids_ref, route_ref, tokens_ref, queries_ref, own_ref, counts_ref, gain_ref, perm_ref, back_ref,
    cache_hbm, fresh_hbm, gate_hbm, up_hbm, down_hbm, out_ref,
    query8, token8, own8, hidden8, kv_all, coef_row,
    gathered, coefs, coef_cols, wide, sums, act, part, crossed, hops, fin, w_in, w_down,
    sem_w, sem_kv, win_send, win_recv, c_send, c_recv, p_send, p_recv, g_send, g_recv, gx_send, gx_recv,
    x_send, x_recv, r_send, r_recv, f_send, f_recv,
):
    n = lax.axis_size("dev_0")
    half_n = n // 2
    core = lax.axis_index("dev_2")
    other = 1 - core
    sgn = 1 - 2 * core
    xy = {"dev_0": lax.axis_index("dev_0"), "dev_1": lax.axis_index("dev_1")}
    pos = [xy[a] for a in RING]
    line = [xy[a] for a in LINE]
    width = gathered.shape[5]
    reqs = tokens_ref.shape[0]
    length = cache_hbm.shape[1]
    span = fresh_hbm.shape[0]
    devices = 2 * n * n
    me = (xy["dev_0"] * n + xy["dev_1"]) * 2 + core

    def wrap(v):
        return lax.rem(v + 2 * n, n)

    def place_of(index):
        index = lax.rem(index + devices, devices)
        return {"dev_0": index // (2 * n), "dev_1": lax.rem(index // 2, n), "dev_2": lax.rem(index, 2)}

    barrier = pltpu.get_barrier_semaphore()
    for step in (-1, 1):
        pl.semaphore_signal(barrier, inc=1, device_id=place_of(me + step), device_id_type=MESH_ID)
    pl.semaphore_signal(barrier, inc=1, device_id={"dev_2": other}, device_id_type=MESH_ID)
    for axis in LINE:
        for j in range(1, n):
            pl.semaphore_signal(
                barrier, inc=1, device_id={axis: wrap(xy[axis] + j)}, device_id_type=MESH_ID
            )
    kv_loads = [
        pltpu.make_async_copy(cache_hbm.at[t], kv_all.at[pl.ds(t * length, length)], sem_kv.at[t])
        for t in range(reqs)
    ]
    kv_loads.append(
        pltpu.make_async_copy(fresh_hbm, kv_all.at[pl.ds(reqs * length, span)], sem_kv.at[reqs])
    )
    for load in kv_loads:
        load.start()
    quarter = 2 * width
    units = gate_hbm.shape[1]
    loads = []
    for h in range(2):
        for q in range(4):
            for k, src in enumerate((gate_hbm, up_hbm)):
                loads.append(
                    pltpu.make_async_copy(
                        src.at[pl.ds(q * quarter + h * width, width)],
                        w_in.at[h, pl.ds(q * width, width), pl.ds(k * units, units)],
                        sem_w.at[(h * 4 + q) * 2 + k],
                    )
                )
    loads.append(pltpu.make_async_copy(down_hbm, w_down, sem_w.at[16]))
    for load in loads:
        load.start()

    query = queries_ref[...].astype(jnp.float32)
    query8[0:reqs] = query
    query8[reqs : 2 * reqs] = query
    token = tokens_ref[...].astype(jnp.float32)
    token8[0:reqs] = token
    token8[reqs : 2 * reqs] = token
    own8[...] = jnp.zeros_like(own8)
    own8[0:reqs] = own_ref[...].astype(jnp.float32)
    kv_all[pl.ds(reqs * length + 2 * span, 16)] = own8[...].astype(jnp.bfloat16)
    rest = reqs * length + 2 * span + 16
    kv_all[pl.ds(rest, kv_all.shape[0] - rest)] = jnp.zeros(
        (kv_all.shape[0] - rest, kv_all.shape[1]), jnp.bfloat16
    )
    lane = lax.broadcasted_iota(jnp.int32, (1, 128), 1)
    coef = jnp.zeros((1, 128), jnp.float32)
    for t in range(reqs):
        for k in range(2):
            coef = coef + jnp.where(lane == t * EXPERTS + ids_ref[t, k], route_ref[t, k], 0.0)
    coef_row[...] = coef
    pl.semaphore_wait(barrier, 2 * (n - 1) + 3)

    pending = []

    def send(src, dst, s_sem, r_sem, where):
        copy = pltpu.make_async_remote_copy(
            src_ref=src, dst_ref=dst, send_sem=s_sem, recv_sem=r_sem,
            device_id=where, device_id_type=MESH_ID,
        )
        copy.start()
        pending.append(copy)
        return copy

    following = send(
        fresh_hbm, kv_all.at[pl.ds(reqs * length + span, span)], win_send.at[0], win_recv.at[0],
        place_of(me - 1),
    )
    static_slot = {o % n: i for i, o in enumerate(OFFSETS)}
    coefs[core, 0, 0] = coef_row[...]
    coef_firsts = [
        send(
            coef_row, coefs.at[core, 0, static_slot[-j % n]], c_send.at[j], c_recv.at[j],
            {"dev_0": wrap(xy["dev_0"] + j)},
        )
        for j in range(1, n)
    ]
    for load in kv_loads:
        load.wait()
    following.wait_recv()
    hidden = token8[...] + attend(
        lens_ref, counts_ref, query8, kv_all, me, reqs, span, length
    )
    hidden8[...] = hidden
    spread_sq = jnp.mean(hidden * hidden, 1, keepdims=True)
    normed = hidden * lax.rsqrt(spread_sq + EPS) * gain_ref[...]
    sub8 = lax.broadcasted_iota(jnp.int32, (8, 4 * width // 2), 0)
    stacked = jnp.concatenate(
        [
            jnp.where(
                sub8 < reqs,
                normed[:, 2 * i * quarter : (2 * i + 1) * quarter],
                normed[:, (2 * i + 1) * quarter : (2 * i + 2) * quarter],
            )
            for i in range(2)
        ],
        0,
    ).astype(jnp.bfloat16)
    for h in range(2):
        gathered[h, core, 0, 0] = stacked[:, h * width : (h + 1) * width]

    ways = ((0, half_n, sgn), (1, half_n - 1, -sgn))
    passing = {}

    def pass_on(s):
        for h in range(2):
            for way, steps, turn in ways:
                if s > 1 and s - 1 <= steps:
                    passing[h, way, s - 1].wait_recv()
                if s <= steps:
                    passing[h, way, s] = send(
                        gathered.at[h, core, 0, slot_at(-turn, s - 1)],
                        gathered.at[h, core, 0, slot_at(-turn, s)],
                        p_send.at[h, way, s - 1], p_recv.at[h, way, s - 1],
                        {LINE[h]: wrap(line[h] + turn)},
                    )

    rounds = {}
    crossing = {}

    def go_round(s, g):
        low, count = GROUPS_OF_BLOCKS[g]
        at = pl.ds(low, count)
        for h in range(2):
            for way, steps, turn in ways:
                if s > 1 and s - 1 <= steps:
                    rounds[h, way, s - 1, g].wait_recv()
                if s <= steps:
                    rounds[h, way, s, g] = send(
                        gathered.at[h, core, slot_at(-turn, s - 1), at],
                        gathered.at[h, core, slot_at(-turn, s), at],
                        g_send.at[h, way, s - 1, g], g_recv.at[h, way, s - 1, g],
                        {RING[h]: wrap(pos[h] + turn)},
                    )
        for h in range(2):
            first, many = slots_of(s - 1)
            ref = gathered.at[h, core, pl.ds(first, many), at]
            crossing[h, s - 1, g] = send(
                ref, ref, gx_send.at[h, s - 1, g], gx_recv.at[h, s - 1, g], {"dev_2": other}
            )

    batch = 2 * n * reqs
    stack = 4 * batch

    def project(d):
        if d == 0:
            for load in loads[:16]:
                load.wait()
        first, many = slots_of(d)
        for h in range(2):
            for g in range(len(GROUPS_OF_BLOCKS)):
                crossing[h, d, g].wait_recv()
            for i in range(many):
                z = gathered[h, :, first + i].reshape(stack, width)
                z = jnp.dot(perm_ref[...], z, preferred_element_type=jnp.float32).astype(jnp.bfloat16)
                for q in range(4):
                    wide[i * batch : (i + 1) * batch, q * width : (q + 1) * width] = z[
                        q * batch : (q + 1) * batch
                    ]
            sums[h, first * batch : (first + many) * batch] = jnp.dot(
                wide[0 : many * batch], w_in[h], preferred_element_type=jnp.float32
            )

    pass_on(1)
    pass_on(2)
    go_round(1, 0)
    for copy in coef_firsts:
        copy.wait_recv()
    coef_seconds = [
        send(
            coefs.at[core, 0], coefs.at[core, static_slot[-j % n]],
            c_send.at[n + j], c_recv.at[n + j], {"dev_1": wrap(xy["dev_1"] + j)},
        )
        for j in range(1, n)
    ]
    pass_on(3)
    go_round(1, 1)
    pass_on(4)
    go_round(2, 0)
    pass_on(5)
    go_round(1, 2)
    for copy in coef_seconds:
        copy.wait_recv()
    coef_both = send(coefs.at[core], coefs.at[core], c_send.at[0], c_recv.at[0], {"dev_2": other})
    go_round(2, 1)
    go_round(3, 0)
    project(0)
    go_round(2, 2)
    go_round(3, 1)
    go_round(4, 0)
    coef_both.wait_recv()
    expert = me // (devices // EXPERTS)
    row8 = lax.broadcasted_iota(jnp.int32, (8, 128), 0)
    lane8 = lax.broadcasted_iota(jnp.int32, (8, 128), 1)
    keep = lane8 == lax.rem(row8, reqs) * EXPERTS + expert
    for r in range(n):
        for c in range(n):
            both = jnp.where(row8 < reqs, coefs[0, r, c], coefs[1, r, c])
            coef_cols[r, c] = jnp.broadcast_to(
                jnp.sum(jnp.where(keep, both, 0.0), 1, keepdims=True), (8, 128)
            )
    project(1)
    go_round(3, 2)
    go_round(4, 1)
    project(2)
    go_round(4, 2)
    go_round(5, 0)
    go_round(5, 1)
    project(3)
    go_round(5, 2)
    project(4)

    for r in range(n):
        both = sums[0, r * batch : (r + 1) * batch] + jnp.concatenate(
            [sums[1, c * batch + r * 8 : c * batch + (r + 1) * 8] for c in range(n)], 0
        )
        gate = both[:, :units]
        up = both[:, units:]
        coef = coef_cols[r].reshape(batch, 128)
        coef = jnp.concatenate([coef] * (units // 128), 1)
        act[r] = (gate / (1.0 + jnp.exp(-gate)) * up * coef).reshape(n, 8, units)
    loads[16].wait()

    crossed_copies = {}

    def descend(d):
        first, many = slots_of(d)
        for h in range(2):
            if h == 0:
                rows = [act[first + i].reshape(batch, units) for i in range(many)]
            else:
                rows = [act[:, first + i].reshape(batch, units) for i in range(many)]
            a = jnp.concatenate(rows, 0).astype(jnp.bfloat16)
            for q in range(4):
                wide[0 : many * batch, q * width : (q + 1) * width] = jnp.dot(
                    a,
                    w_down[:, q * quarter + h * width : q * quarter + (h + 1) * width],
                    preferred_element_type=jnp.float32,
                ).astype(jnp.bfloat16)
            for i in range(many):
                z = jnp.concatenate(
                    [
                        wide[i * batch : (i + 1) * batch, q * width : (q + 1) * width]
                        for q in range(4)
                    ],
                    0,
                )
                z = jnp.dot(back_ref[...], z, preferred_element_type=jnp.float32)
                part[h, :, first + i] = z.astype(jnp.bfloat16).reshape(2, n, 16, width)
            at = pl.ds(first, many)
            crossed_copies[h, d] = send(
                part.at[h, other, at], crossed.at[h, at], x_send.at[h, d], x_recv.at[h, d],
                {"dev_2": other},
            )

    held = {}

    def collect(k):
        distance = half_n + 1 - k
        for h in range(2):
            crossed_copies[h, distance].wait_recv()
        for g in (2, 1, 0):
            low, count = GROUPS_OF_BLOCKS[g]
            at = pl.ds(low, count)
            for h in range(2):
                for way, steps, turn in ways:
                    s = k - (half_n - steps)
                    if s < 1:
                        continue
                    slot = slot_at(turn, distance)
                    total = part[h, core, slot, at].astype(jnp.float32) + crossed[h, slot, at].astype(
                        jnp.float32
                    )
                    if s > 1:
                        held[h, way, s - 1, g].wait_recv()
                        total = total + hops[h, way, s - 2, at].astype(jnp.float32)
                    part[h, core, slot, at] = total.astype(jnp.bfloat16)
                    held[h, way, s, g] = send(
                        part.at[h, core, slot, at], hops.at[h, way, s - 1, at],
                        r_send.at[h, way, s - 1, g], r_recv.at[h, way, s - 1, g],
                        {RING[h]: wrap(pos[h] + turn)},
                    )

    def collect_own(g):
        low, count = GROUPS_OF_BLOCKS[g]
        at = pl.ds(low, count)
        for h in range(2):
            total = part[h, core, 0, at].astype(jnp.float32) + crossed[h, 0, at].astype(jnp.float32)
            for way, steps, turn in ways:
                held[h, way, steps, g].wait_recv()
                total = total + hops[h, way, steps - 1, at].astype(jnp.float32)
            part[h, core, 0, at] = total.astype(jnp.bfloat16)

    finals = {}

    def finish(k):
        distance = half_n + 1 - k
        for h in range(2):
            for way, steps, turn in ways:
                s = k - (half_n - steps)
                if s < 1:
                    continue
                slot = slot_at(turn, distance)
                if s > 1:
                    finals[h, way, s - 1].wait_recv()
                    part[h, core, 0, slot] = (
                        part[h, core, 0, slot].astype(jnp.float32)
                        + fin[h, way, s - 2].astype(jnp.float32)
                    ).astype(jnp.bfloat16)
                finals[h, way, s] = send(
                    part.at[h, core, 0, slot], fin.at[h, way, s - 1],
                    f_send.at[h, way, s - 1], f_recv.at[h, way, s - 1],
                    {LINE[h]: wrap(line[h] + turn)},
                )

    descend(4)
    descend(3)
    collect(1)
    descend(2)
    collect(2)
    descend(1)
    collect(3)
    descend(0)
    collect(4)
    for h in range(2):
        crossed_copies[h, 0].wait_recv()
    collect_own(2)
    finish(1)
    collect_own(1)
    finish(2)
    collect_own(0)
    finish(3)
    finish(4)
    totals = []
    for h in range(2):
        total = part[h, core, 0, 0].astype(jnp.float32)
        for way, steps, turn in ways:
            finals[h, way, steps].wait_recv()
            total = total + fin[h, way, steps - 1].astype(jnp.float32)
        totals.append(total)
    moe = jnp.concatenate(totals, 1)
    pieces = []
    for i in range(2):
        pieces.append(moe[8 * i : 8 * i + 8])
        pieces.append(pltpu.roll(moe[8 * i : 8 * i + 8], reqs, 0))
    final = hidden8[...] + jnp.concatenate(pieces, 1)
    out_ref[...] = final[0:reqs].astype(jnp.bfloat16)
    for copy in pending:
        copy.wait_send()


def per_device(
    tokens,
    queries,
    token_kv,
    kv_cache,
    context_lengths,
    fresh_kv,
    block_counts,
    expert_ids,
    route_weights,
    norm_gain,
    w_gate,
    w_up,
    w_down,
):
    n = lax.axis_size("dev_0")
    reqs, full = tokens.shape
    width = full // 8
    units = w_gate.shape[1]
    rows = 2 * n * n * reqs
    size = 4 * 2 * n * reqs
    r = jnp.arange(size, dtype=jnp.int32)
    q, b, c, t = r // (size // 4), (r // (2 * reqs)) % n, (r // reqs) % 2, r % reqs
    source = c * (size // 2) + b * 16 + q * reqs + t
    perm = (source[:, None] == r[None, :]).astype(jnp.bfloat16)
    back = perm.T
    vmem = pl.BlockSpec(memory_space=pltpu.VMEM)
    smem = pl.BlockSpec(memory_space=pltpu.SMEM)
    anyspace = pl.BlockSpec(memory_space=pl.ANY)
    bf = jnp.bfloat16
    f32 = jnp.float32
    dma = pltpu.SemaphoreType.DMA
    half_n = n // 2
    keys = reqs * kv_cache.shape[1] + 2 * fresh_kv.shape[0] + 128
    return pl.pallas_call(
        layer_kernel,
        out_shape=jax.ShapeDtypeStruct(tokens.shape, bf),
        in_specs=[smem] * 3 + [vmem] * 7 + [anyspace] * 5,
        out_specs=vmem,
        scratch_shapes=[
            pltpu.VMEM((2 * reqs, full), f32),
            pltpu.VMEM((2 * reqs, full), f32),
            pltpu.VMEM((16, token_kv.shape[1]), f32),
            pltpu.VMEM((2 * reqs, full), f32),
            pltpu.VMEM((keys, token_kv.shape[1]), bf),
            pltpu.VMEM((1, 128), f32),
            pltpu.VMEM((2, 2, n, n, 16, width), bf),
            pltpu.VMEM((2, n, n, 1, 128), f32),
            pltpu.VMEM((n, n, 8, 128), f32),
            pltpu.VMEM((4 * n * reqs, full // 2), bf),
            pltpu.VMEM((2, rows, 2 * units), f32),
            pltpu.VMEM((n, n, 8, units), f32),
            pltpu.VMEM((2, 2, n, n, 16, width), bf),
            pltpu.VMEM((2, n, n, 16, width), bf),
            pltpu.VMEM((2, 2, half_n, n, 16, width), bf),
            pltpu.VMEM((2, 2, half_n, 16, width), bf),
            pltpu.VMEM((2, full // 2, 2 * units), bf),
            pltpu.VMEM(w_down.shape, bf),
            dma((17,)),
            dma((reqs + 1,)),
            dma((1,)), dma((1,)),
            dma((2 * n,)), dma((2 * n,)),
            dma((2, 2, half_n)), dma((2, 2, half_n)),
            dma((2, 2, half_n, 3)), dma((2, 2, half_n, 3)),
            dma((2, half_n + 1, 3)), dma((2, half_n + 1, 3)),
            dma((2, half_n + 1)), dma((2, half_n + 1)),
            dma((2, 2, half_n, 3)), dma((2, 2, half_n, 3)),
            dma((2, 2, half_n)), dma((2, 2, half_n)),
        ],
        compiler_params=pltpu.CompilerParams(
            collective_id=0, has_side_effects=True, vmem_limit_bytes=60 * 1024 * 1024
        ),
    )(
        context_lengths, expert_ids, route_weights, tokens, queries, token_kv,
        block_counts.reshape(1, -1), norm_gain.reshape(1, -1), perm, back,
        kv_cache, fresh_kv, w_gate, w_up, w_down,
    )


def solution(mesh):
    split = Mesh(
        mesh.devices.reshape(mesh.shape["groups"], 8, 8, 2), ("groups", "dev_0", "dev_1", "dev_2")
    )
    return jax.shard_map(
        per_device,
        mesh=split,
        in_specs=(
            P(GROUPS_DEV, None),
            P(GROUPS_DEV, None),
            P(GROUPS_DEV, None),
            P(GROUPS_DEV, None, None),
            P(GROUPS_DEV),
            P(GROUPS_DEV, None),
            P("groups"),
            P(GROUPS_DEV, None),
            P(GROUPS_DEV, None),
            P(),
            P(None, DEV),
            P(None, DEV),
            P(DEV, None),
        ),
        out_specs=P(GROUPS_DEV, None),
        check_vma=False,
    )
```

```python
import math

import jax
import jax.numpy as jnp
from jax import lax
from jax.sharding import Mesh
from jax.sharding import PartitionSpec as P
from jax.experimental import pallas as pl
from jax.experimental.pallas import tpu as pltpu

QH = 48
KVH = 8
HD = 128
EXPERTS = 4
BLOCK = 16
DEV = ("dev_0", "dev_1", "dev_2")
GROUPS_DEV = ("groups", "dev_0", "dev_1", "dev_2")


EPS = 1e-05
NEG = -1e30


MESH_ID = pl.DeviceIdType.MESH
RING = ("dev_1", "dev_0")
LINE = ("dev_0", "dev_1")
OFFSETS = (0, 1, -1, 2, -2, 3, -3, 4)
GROUPS_OF_BLOCKS = ((0, 3), (3, 2), (5, 3))
NEAR_AND_FAR = ((0, 5), (5, 3))


def slot_at(sign, distance):
    if distance in (0, 4):
        return 2 * distance - distance // 4
    return 2 * distance - (1 + sign) // 2


def slots_of(distance):
    if distance == 0:
        return (0, 1)
    return (2 * distance - 1, 1 if distance == 4 else 2)


def query_rows(query8, reqs):
    sub8 = lax.broadcasted_iota(jnp.int32, (8, HD), 0)
    group = QH // KVH
    tiles = []
    for h in range(0, QH, 2):
        a = query8[:, h * HD : (h + 1) * HD]
        b = query8[:, (h + 1) * HD : (h + 2) * HD]
        tiles.append(jnp.where(sub8 < reqs, a, b))
    return [
        jnp.concatenate(tiles[k * group // 2 : (k + 1) * group // 2], 0).astype(jnp.bfloat16)
        for k in range(KVH)
    ]


def scores_of(q, keys):
    return lax.dot_general(
        q, keys, (((1,), (1,)), ((), ())), preferred_element_type=jnp.float32
    ) * (1.0 / math.sqrt(HD))


def attend_held(lens_ref, queries, kv_all, reqs, length, held):
    half = KVH * HD
    rows = queries[0].shape[0]
    key = lax.broadcasted_iota(jnp.int32, (1, held), 1)
    owner = jnp.full((1, held), -1, jnp.int32)
    for t in range(reqs):
        place = key - t * length
        mine = (place >= 0) & (place < length) & (place < lens_ref[0:1, t : t + 1])
        owner = jnp.where(mine, t, owner)
    place = key - reqs * length
    owner = jnp.where((place >= 0) & (place < reqs), place, owner)
    row = lax.rem(lax.broadcasted_iota(jnp.int32, (rows, held), 0), reqs)
    valid = row == owner
    states = []
    for k in range(KVH):
        s = scores_of(queries[k], kv_all[0:held, k * HD : (k + 1) * HD])
        s = jnp.where(valid, s, NEG)
        top = jnp.max(s, 1, keepdims=True)
        e = jnp.exp(s - top)
        total = jnp.sum(e, 1, keepdims=True)
        mixed = jnp.dot(
            e.astype(jnp.bfloat16),
            kv_all[0:held, half + k * HD : half + (k + 1) * HD],
            preferred_element_type=jnp.float32,
        )
        states.append((top, total, mixed))
    return states


def heads_aside(mixed, reqs):
    sub8 = lax.broadcasted_iota(jnp.int32, (8, HD), 0)
    parts = []
    for piece_of in mixed:
        for i in range(QH // KVH // 2):
            piece = piece_of[8 * i : 8 * i + 8]
            turned = pltpu.roll(piece, reqs, 0)
            parts.append(jnp.where(sub8 < reqs, piece, turned))
            parts.append(jnp.where(sub8 < reqs, turned, piece))
    return jnp.concatenate(parts, 1)


def attend_window(counts_ref, queries, states, kv_all, me, reqs, span, held):
    half = KVH * HD
    rows = queries[0].shape[0]
    counts = counts_ref[...]
    lane = lax.broadcasted_iota(jnp.int32, counts.shape, 1)
    offset = jnp.sum(jnp.where(lane < me, counts, 0), 1, keepdims=True)
    taken = jnp.sum(jnp.where(lane == me, counts, 0), 1, keepdims=True)
    first = offset * BLOCK - me * span
    stop = first + taken * BLOCK
    place = lax.broadcasted_iota(jnp.int32, (rows, 2 * span), 1)
    row = lax.rem(lax.broadcasted_iota(jnp.int32, (rows, 2 * span), 0), reqs)
    live = (row == 0) & (place >= first) & (place < stop)
    parts = []
    for k in range(KVH):
        top, total, mixed = states[k]
        s = scores_of(queries[k], kv_all[held : held + 2 * span, k * HD : (k + 1) * HD])
        s = jnp.where(live, s, NEG)
        new = jnp.maximum(top, jnp.max(s, 1, keepdims=True))
        fade = jnp.exp(top - new)
        e = jnp.exp(s - new)
        total = total * fade + jnp.sum(e, 1, keepdims=True)
        mixed = mixed * fade + jnp.dot(
            e.astype(jnp.bfloat16),
            kv_all[held : held + 2 * span, half + k * HD : half + (k + 1) * HD],
            preferred_element_type=jnp.float32,
        )
        parts.append(mixed / total)
    return heads_aside(parts, reqs)


def layer_kernel(
    lens_hbm, ids_hbm, route_hbm, tokens_hbm, queries_hbm, own_hbm, counts_hbm, gain_hbm,
    cache_hbm, fresh_hbm, gate_hbm, up_hbm, down_hbm, out_ref,
    lens_ref, ids_ref, route_ref, tokens_ref, queries_ref, own_ref, counts_ref, gain_ref,
    query8, token8, own8, hidden8, kv_all, coef_row, perm_ref, back_ref,
    gathered, coefs, coef_cols, wide, sums, act, part, crossed, hops, fin, w_in, w_down,
    sem_w, sem_kv, sem_in, win_send, win_recv, c_send, c_recv, p_send, p_recv, g_send, g_recv, gx_send, gx_recv,
    x_send, x_recv, r_send, r_recv, f_send, f_recv,
):
    n = lax.axis_size("dev_0")
    half_n = n // 2
    core = lax.axis_index("dev_2")
    other = 1 - core
    sgn = 1 - 2 * core
    xy = {"dev_0": lax.axis_index("dev_0"), "dev_1": lax.axis_index("dev_1")}
    pos = [xy[a] for a in RING]
    line = [xy[a] for a in LINE]
    width = gathered.shape[6]
    reqs = tokens_hbm.shape[0]
    length = cache_hbm.shape[1]
    span = fresh_hbm.shape[0]
    devices = 2 * n * n
    held = reqs * length + 128
    me = (xy["dev_0"] * n + xy["dev_1"]) * 2 + core

    def wrap(v):
        return lax.rem(v + 2 * n, n)

    def place_of(index):
        index = lax.rem(index + devices, devices)
        return {"dev_0": index // (2 * n), "dev_1": lax.rem(index // 2, n), "dev_2": lax.rem(index, 2)}

    barrier = pltpu.get_barrier_semaphore()
    for step in (-1, 1):
        pl.semaphore_signal(barrier, inc=1, device_id=place_of(me + step), device_id_type=MESH_ID)
    pl.semaphore_signal(barrier, inc=1, device_id={"dev_2": other}, device_id_type=MESH_ID)
    for axis in LINE:
        for j in range(1, n):
            pl.semaphore_signal(
                barrier, inc=1, device_id={axis: wrap(xy[axis] + j)}, device_id_type=MESH_ID
            )
    kv_loads = [
        pltpu.make_async_copy(cache_hbm.at[t], kv_all.at[pl.ds(t * length, length)], sem_kv.at[t])
        for t in range(reqs)
    ]
    kv_loads.append(
        pltpu.make_async_copy(fresh_hbm, kv_all.at[pl.ds(held, span)], sem_kv.at[reqs])
    )
    small = (
        (queries_hbm, queries_ref), (tokens_hbm, tokens_ref), (own_hbm, own_ref), (lens_hbm, lens_ref),
        (ids_hbm, ids_ref), (route_hbm, route_ref), (counts_hbm, counts_ref), (gain_hbm, gain_ref),
    )
    small_loads = [
        pltpu.make_async_copy(src, dst, sem_in.at[i]) for i, (src, dst) in enumerate(small)
    ]
    for load in small_loads + kv_loads:
        load.start()
    quarter = 2 * width
    units = gate_hbm.shape[1]
    loads = []
    for h in range(2):
        for q in range(4):
            for k, src in enumerate((gate_hbm, up_hbm)):
                loads.append(
                    pltpu.make_async_copy(
                        src.at[pl.ds(q * quarter + h * width, width)],
                        w_in.at[h, pl.ds(q * width, width), pl.ds(k * units, units)],
                        sem_w.at[(h * 4 + q) * 2 + k],
                    )
                )
    loads.append(pltpu.make_async_copy(down_hbm, w_down, sem_w.at[16]))
    for load in loads:
        load.start()

    for load in small_loads:
        load.wait()
    query = queries_ref[...].astype(jnp.float32)
    query8[0:reqs] = query
    query8[reqs : 2 * reqs] = query
    token = tokens_ref[...].astype(jnp.float32)
    token8[0:reqs] = token
    token8[reqs : 2 * reqs] = token
    own8[...] = jnp.zeros_like(own8)
    own8[0:reqs] = own_ref[...].astype(jnp.float32)
    kv_all[pl.ds(reqs * length, 16)] = own8[...].astype(jnp.bfloat16)
    kv_all[pl.ds(reqs * length + 16, 112)] = jnp.zeros((112, kv_all.shape[1]), jnp.bfloat16)
    lane = lax.broadcasted_iota(jnp.int32, (1, 128), 1)
    coef = jnp.zeros((1, 128), jnp.float32)
    for t in range(reqs):
        for k in range(2):
            coef = coef + jnp.where(lane == t * EXPERTS + ids_ref[k : k + 1, t : t + 1], route_ref[k : k + 1, t : t + 1], 0.0)
    coef_row[...] = coef
    kv_loads[reqs].wait()
    pl.semaphore_wait(barrier, 2 * (n - 1) + 3)

    pending = []

    def send(src, dst, s_sem, r_sem, where):
        copy = pltpu.make_async_remote_copy(
            src_ref=src, dst_ref=dst, send_sem=s_sem, recv_sem=r_sem,
            device_id=where, device_id_type=MESH_ID,
        )
        copy.start()
        pending.append(copy)
        return copy

    following = send(
        kv_all.at[pl.ds(held, span)], kv_all.at[pl.ds(held + span, span)], win_send.at[0], win_recv.at[0],
        place_of(me - 1),
    )
    static_slot = {o % n: i for i, o in enumerate(OFFSETS)}
    coefs[core, 0, 0] = coef_row[...]
    coef_firsts = [
        send(
            coef_row, coefs.at[core, 0, static_slot[-j % n]], c_send.at[j], c_recv.at[j],
            {"dev_0": wrap(xy["dev_0"] + j)},
        )
        for j in range(1, n)
    ]
    size = perm_ref.shape[0]

    def parts_of(r):
        return r // (size // 4), lax.rem(r // (2 * reqs), n), lax.rem(r // reqs, 2), lax.rem(r, reqs)

    def stacked_row(r):
        q, b, c, t = parts_of(r)
        return c * (size // 2) + b * 16 + q * reqs + t

    def waved_row(r):
        q, b, c, t = parts_of(r)
        wave = 1 - t // 2
        return wave * (size // 2) + c * (size // 4) + b * 8 + lax.rem(t, 2) * 4 + q

    row = lax.broadcasted_iota(jnp.int32, (size, 1), 0)
    column = lax.broadcasted_iota(jnp.int32, (1, size), 1)
    perm_ref[...] = (waved_row(row) == column).astype(jnp.float32).astype(jnp.bfloat16)
    back_ref[...] = (row == stacked_row(column)).astype(jnp.float32).astype(jnp.bfloat16)
    for load in kv_loads[:reqs]:
        load.wait()
    queries = query_rows(query8, reqs)
    states = attend_held(lens_ref, queries, kv_all, reqs, length, held)
    token = token8[...]
    gain = gain_ref[...]
    row8 = lax.broadcasted_iota(jnp.int32, (8, quarter), 0)

    def normed_of(hidden):
        mean = jnp.mean(hidden * hidden, 1, keepdims=True)
        return hidden * lax.rsqrt(mean + EPS) * gain

    def put(wave, normed):
        block = jnp.zeros((8, quarter), jnp.float32)
        for i in range(2):
            t = 2 * (1 - wave) + i
            for q in range(4):
                line_of = jnp.broadcast_to(
                    normed[t : t + 1, q * quarter : (q + 1) * quarter], (8, quarter)
                )
                block = jnp.where(row8 == i * 4 + q, line_of, block)
        block = block.astype(jnp.bfloat16)
        for h in range(2):
            gathered[wave, h, core, 0, 0] = block[:, h * width : (h + 1) * width]

    passing = {}

    def depart(wave):
        for slot in range(1, n):
            for h in range(2):
                offset = OFFSETS[slot]
                passing[wave, h, slot] = send(
                    gathered.at[wave, h, core, 0, 0],
                    gathered.at[wave, h, core, 0, static_slot[-offset % n]],
                    p_send.at[wave, h, slot], p_recv.at[wave, h, slot],
                    {LINE[h]: wrap(line[h] + offset)},
                )

    early = heads_aside([mixed / total for _, total, mixed in states], reqs)
    put(0, normed_of(token + early))
    depart(0)
    following.wait_recv()
    hidden = token + attend_window(
        counts_ref, queries, states, kv_all, me, reqs, span, held
    )
    hidden8[...] = hidden
    put(1, normed_of(hidden))
    depart(1)

    ways = ((0, half_n, sgn), (1, half_n - 1, -sgn))
    def arrive(wave, g):
        low, count = NEAR_AND_FAR[g]
        for slot in range(max(low, 1), low + count):
            for h in range(2):
                passing[wave, h, slot].wait_recv()

    rounds = {}
    crossing = {}

    def go_round(wave, s, g):
        low, count = NEAR_AND_FAR[g]
        at = pl.ds(low, count)
        for h in range(2):
            for way, steps, turn in ways:
                if s > 1 and s - 1 <= steps:
                    rounds[wave, h, way, s - 1, g].wait_recv()
                if s <= steps:
                    rounds[wave, h, way, s, g] = send(
                        gathered.at[wave, h, core, slot_at(-turn, s - 1), at],
                        gathered.at[wave, h, core, slot_at(-turn, s), at],
                        g_send.at[wave, h, way, s - 1, g], g_recv.at[wave, h, way, s - 1, g],
                        {RING[h]: wrap(pos[h] + turn)},
                    )
        for h in range(2):
            first, many = slots_of(s - 1)
            ref = gathered.at[wave, h, core, pl.ds(first, many), at]
            crossing[wave, h, s - 1, g] = send(
                ref, ref, gx_send.at[wave, h, s - 1, g], gx_recv.at[wave, h, s - 1, g],
                {"dev_2": other},
            )

    batch = 2 * n * reqs
    stack = 4 * batch

    def project(d):
        if d == 0:
            for load in loads[:16]:
                load.wait()
        first, many = slots_of(d)
        for h in range(2):
            for wave in range(2):
                for g in range(len(NEAR_AND_FAR)):
                    crossing[wave, h, d, g].wait_recv()
            for i in range(many):
                z = gathered[:, h, :, first + i].reshape(stack, width)
                z = jnp.dot(perm_ref[...], z, preferred_element_type=jnp.float32).astype(jnp.bfloat16)
                for q in range(4):
                    wide[i * batch : (i + 1) * batch, q * width : (q + 1) * width] = z[
                        q * batch : (q + 1) * batch
                    ]
            sums[h, first * batch : (first + many) * batch] = jnp.dot(
                wide[0 : many * batch], w_in[h], preferred_element_type=jnp.float32
            )

    arrive(0, 0)
    go_round(0, 1, 0)
    arrive(0, 1)
    go_round(0, 1, 1)
    for copy in coef_firsts:
        copy.wait_recv()
    coef_seconds = [
        send(
            coefs.at[core, 0], coefs.at[core, static_slot[-j % n]],
            c_send.at[n + j], c_recv.at[n + j], {"dev_1": wrap(xy["dev_1"] + j)},
        )
        for j in range(1, n)
    ]
    go_round(0, 2, 0)
    arrive(1, 0)
    go_round(1, 1, 0)
    go_round(0, 2, 1)
    arrive(1, 1)
    go_round(1, 1, 1)
    for copy in coef_seconds:
        copy.wait_recv()
    coef_both = send(coefs.at[core], coefs.at[core], c_send.at[0], c_recv.at[0], {"dev_2": other})
    go_round(0, 3, 0)
    go_round(1, 2, 0)
    project(0)
    go_round(0, 3, 1)
    go_round(1, 2, 1)
    go_round(0, 4, 0)
    go_round(1, 3, 0)
    coef_both.wait_recv()
    expert = me // (devices // EXPERTS)
    row8 = lax.broadcasted_iota(jnp.int32, (8, 128), 0)
    lane8 = lax.broadcasted_iota(jnp.int32, (8, 128), 1)
    keep = lane8 == lax.rem(row8, reqs) * EXPERTS + expert
    for r in range(n):
        for c in range(n):
            both = jnp.where(row8 < reqs, coefs[0, r, c], coefs[1, r, c])
            coef_cols[r, c] = jnp.broadcast_to(
                jnp.sum(jnp.where(keep, both, 0.0), 1, keepdims=True), (8, 128)
            )
    project(1)
    go_round(0, 4, 1)
    go_round(1, 3, 1)
    go_round(0, 5, 0)
    go_round(1, 4, 0)
    project(2)
    go_round(0, 5, 1)
    go_round(1, 4, 1)
    go_round(1, 5, 0)
    project(3)
    go_round(1, 5, 1)
    project(4)

    for r in range(n):
        both = sums[0, r * batch : (r + 1) * batch] + jnp.concatenate(
            [sums[1, c * batch + r * 8 : c * batch + (r + 1) * 8] for c in range(n)], 0
        )
        gate = both[:, :units]
        up = both[:, units:]
        coef = coef_cols[r].reshape(batch, 128)
        coef = jnp.concatenate([coef] * (units // 128), 1)
        act[r] = (gate / (1.0 + jnp.exp(-gate)) * up * coef).reshape(n, 8, units)
    loads[16].wait()

    crossed_copies = {}

    def descend(d):
        first, many = slots_of(d)
        for h in range(2):
            if h == 0:
                rows = [act[first + i].reshape(batch, units) for i in range(many)]
            else:
                rows = [act[:, first + i].reshape(batch, units) for i in range(many)]
            a = jnp.concatenate(rows, 0).astype(jnp.bfloat16)
            for q in range(4):
                wide[0 : many * batch, q * width : (q + 1) * width] = jnp.dot(
                    a,
                    w_down[:, q * quarter + h * width : q * quarter + (h + 1) * width],
                    preferred_element_type=jnp.float32,
                ).astype(jnp.bfloat16)
            for i in range(many):
                z = jnp.concatenate(
                    [
                        wide[i * batch : (i + 1) * batch, q * width : (q + 1) * width]
                        for q in range(4)
                    ],
                    0,
                )
                z = jnp.dot(back_ref[...], z, preferred_element_type=jnp.float32)
                part[h, :, first + i] = z.astype(jnp.bfloat16).reshape(2, n, 16, width)
            at = pl.ds(first, many)
            crossed_copies[h, d] = send(
                part.at[h, other, at], crossed.at[h, at], x_send.at[h, d], x_recv.at[h, d],
                {"dev_2": other},
            )

    holding = {}

    def collect(k):
        distance = half_n + 1 - k
        for h in range(2):
            crossed_copies[h, distance].wait_recv()
        for g in (2, 1, 0):
            low, count = GROUPS_OF_BLOCKS[g]
            at = pl.ds(low, count)
            for h in range(2):
                for way, steps, turn in ways:
                    s = k - (half_n - steps)
                    if s < 1:
                        continue
                    slot = slot_at(turn, distance)
                    total = part[h, core, slot, at].astype(jnp.float32) + crossed[h, slot, at].astype(
                        jnp.float32
                    )
                    if s > 1:
                        holding[h, way, s - 1, g].wait_recv()
                        total = total + hops[h, way, s - 2, at].astype(jnp.float32)
                    part[h, core, slot, at] = total.astype(jnp.bfloat16)
                    holding[h, way, s, g] = send(
                        part.at[h, core, slot, at], hops.at[h, way, s - 1, at],
                        r_send.at[h, way, s - 1, g], r_recv.at[h, way, s - 1, g],
                        {RING[h]: wrap(pos[h] + turn)},
                    )

    def collect_own(g):
        low, count = GROUPS_OF_BLOCKS[g]
        at = pl.ds(low, count)
        for h in range(2):
            total = part[h, core, 0, at].astype(jnp.float32) + crossed[h, 0, at].astype(jnp.float32)
            for way, steps, turn in ways:
                holding[h, way, steps, g].wait_recv()
                total = total + hops[h, way, steps - 1, at].astype(jnp.float32)
            part[h, core, 0, at] = total.astype(jnp.bfloat16)
        for slot in reversed(range(max(low, 1), low + count)):
            for h in range(2):
                finals.append(
                    send(
                        part.at[h, core, 0, slot], fin.at[h, slot], f_send.at[h, slot], f_recv.at[h, slot],
                        {LINE[h]: wrap(line[h] + OFFSETS[slot])},
                    )
                )

    finals = []
    descend(4)
    descend(3)
    collect(1)
    descend(2)
    collect(2)
    descend(1)
    collect(3)
    descend(0)
    collect(4)
    for h in range(2):
        crossed_copies[h, 0].wait_recv()
    collect_own(2)
    collect_own(1)
    collect_own(0)
    for copy in finals:
        copy.wait_recv()
    totals = []
    for h in range(2):
        total = part[h, core, 0, 0].astype(jnp.float32)
        for slot in range(1, n):
            total = total + fin[h, slot].astype(jnp.float32)
        totals.append(total)
    moe = jnp.concatenate(totals, 1)
    pieces = []
    for i in range(2):
        pieces.append(moe[8 * i : 8 * i + 8])
        pieces.append(pltpu.roll(moe[8 * i : 8 * i + 8], reqs, 0))
    final = hidden8[...] + jnp.concatenate(pieces, 1)
    out_ref[...] = final[0:reqs]
    for copy in pending:
        copy.wait_send()


def per_device(
    tokens,
    queries,
    token_kv,
    kv_cache,
    context_lengths,
    fresh_kv,
    block_counts,
    expert_ids,
    route_weights,
    norm_gain,
    w_gate,
    w_up,
    w_down,
):
    n = lax.axis_size("dev_0")
    reqs, full = tokens.shape
    width = full // 8
    units = w_gate.shape[1]
    rows = 2 * n * n * reqs
    size = 4 * 2 * n * reqs
    vmem = pl.BlockSpec(memory_space=pltpu.VMEM)
    anyspace = pl.BlockSpec(memory_space=pl.ANY)
    bf = jnp.bfloat16
    f32 = jnp.float32
    dma = pltpu.SemaphoreType.DMA
    half_n = n // 2
    keys = reqs * kv_cache.shape[1] + 2 * fresh_kv.shape[0] + 128
    result = pl.pallas_call(
        layer_kernel,
        out_shape=jax.ShapeDtypeStruct(tokens.shape, f32),
        in_specs=[anyspace] * 13,
        out_specs=vmem,
        scratch_shapes=[
            pltpu.VMEM((1, reqs), jnp.int32),
            pltpu.VMEM((2, reqs), jnp.int32),
            pltpu.VMEM((2, reqs), f32),
            pltpu.VMEM(tokens.shape, bf),
            pltpu.VMEM(queries.shape, bf),
            pltpu.VMEM(token_kv.shape, bf),
            pltpu.VMEM((1, block_counts.shape[0]), jnp.int32),
            pltpu.VMEM((1, full), f32),
            pltpu.VMEM((2 * reqs, full), f32),
            pltpu.VMEM((2 * reqs, full), f32),
            pltpu.VMEM((16, token_kv.shape[1]), f32),
            pltpu.VMEM((2 * reqs, full), f32),
            pltpu.VMEM((keys, token_kv.shape[1]), bf),
            pltpu.VMEM((1, 128), f32),
            pltpu.VMEM((size, size), bf),
            pltpu.VMEM((size, size), bf),
            pltpu.VMEM((2, 2, 2, n, n, 8, width), bf),
            pltpu.VMEM((2, n, n, 1, 128), f32),
            pltpu.VMEM((n, n, 8, 128), f32),
            pltpu.VMEM((4 * n * reqs, full // 2), bf),
            pltpu.VMEM((2, rows, 2 * units), f32),
            pltpu.VMEM((n, n, 8, units), f32),
            pltpu.VMEM((2, 2, n, n, 16, width), bf),
            pltpu.VMEM((2, n, n, 16, width), bf),
            pltpu.VMEM((2, 2, half_n, n, 16, width), bf),
            pltpu.VMEM((2, n, 16, width), bf),
            pltpu.VMEM((2, full // 2, 2 * units), bf),
            pltpu.VMEM(w_down.shape, bf),
            dma((17,)),
            dma((reqs + 1,)),
            dma((8,)),
            dma((1,)), dma((1,)),
            dma((2 * n,)), dma((2 * n,)),
            dma((2, 2, n)), dma((2, 2, n)),
            dma((2, 2, 2, half_n, 2)), dma((2, 2, 2, half_n, 2)),
            dma((2, 2, half_n + 1, 2)), dma((2, 2, half_n + 1, 2)),
            dma((2, half_n + 1)), dma((2, half_n + 1)),
            dma((2, 2, half_n, 3)), dma((2, 2, half_n, 3)),
            dma((2, n)), dma((2, n)),
        ],
        compiler_params=pltpu.CompilerParams(
            collective_id=0, has_side_effects=True, vmem_limit_bytes=60 * 1024 * 1024
        ),
    )(
        context_lengths.reshape(1, -1), expert_ids.T, route_weights.T, tokens, queries, token_kv,
        block_counts.reshape(1, -1), norm_gain.reshape(1, -1),
        kv_cache, fresh_kv, w_gate, w_up, w_down,
    )
    return result.astype(bf)


def solution(mesh):
    split = Mesh(
        mesh.devices.reshape(mesh.shape["groups"], 8, 8, 2), ("groups", "dev_0", "dev_1", "dev_2")
    )
    return jax.shard_map(
        per_device,
        mesh=split,
        in_specs=(
            P(GROUPS_DEV, None),
            P(GROUPS_DEV, None),
            P(GROUPS_DEV, None),
            P(GROUPS_DEV, None, None),
            P(GROUPS_DEV),
            P(GROUPS_DEV, None),
            P("groups"),
            P(GROUPS_DEV, None),
            P(GROUPS_DEV, None),
            P(),
            P(None, DEV),
            P(None, DEV),
            P(DEV, None),
        ),
        out_specs=P(GROUPS_DEV, None),
        check_vma=False,
    )
```

```python
import math

import jax
import jax.numpy as jnp
from jax import lax
from jax.sharding import Mesh
from jax.sharding import PartitionSpec as P
from jax.experimental import pallas as pl
from jax.experimental.pallas import tpu as pltpu

QH = 48
KVH = 8
HD = 128
EXPERTS = 4
BLOCK = 16
DEV = ("dev_0", "dev_1", "dev_2")
GROUPS_DEV = ("groups", "dev_0", "dev_1", "dev_2")


EPS = 1e-05
NEG = -1e30


MESH_ID = pl.DeviceIdType.MESH
RING = ("dev_1", "dev_0")
LINE = ("dev_0", "dev_1")
OFFSETS = (0, 1, -1, 2, -2, 3, -3, 4)
GROUPS_OF_BLOCKS = ((0, 3), (3, 2), (5, 3))
NEAR_AND_FAR = ((0, 5), (5, 3))


def slot_at(sign, distance):
    if distance in (0, 4):
        return 2 * distance - distance // 4
    return 2 * distance - (1 + sign) // 2


def slots_of(distance):
    if distance == 0:
        return (0, 1)
    return (2 * distance - 1, 1 if distance == 4 else 2)


def query_rows(query8, reqs):
    sub8 = lax.broadcasted_iota(jnp.int32, (8, HD), 0)
    group = QH // KVH
    tiles = []
    for h in range(0, QH, 2):
        a = query8[:, h * HD : (h + 1) * HD]
        b = query8[:, (h + 1) * HD : (h + 2) * HD]
        tiles.append(jnp.where(sub8 < reqs, a, b))
    return [
        jnp.concatenate(tiles[k * group // 2 : (k + 1) * group // 2], 0).astype(jnp.bfloat16)
        for k in range(KVH)
    ]


def scores_of(q, keys):
    return lax.dot_general(
        q, keys, (((1,), (1,)), ((), ())), preferred_element_type=jnp.float32
    ) * (1.0 / math.sqrt(HD))


def attend_held(lens_ref, queries, kv_all, reqs, length, held):
    half = KVH * HD
    rows = queries[0].shape[0]
    key = lax.broadcasted_iota(jnp.int32, (1, held), 1)
    owner = jnp.full((1, held), -1, jnp.int32)
    for t in range(reqs):
        place = key - t * length
        mine = (place >= 0) & (place < length) & (place < lens_ref[0:1, t : t + 1])
        owner = jnp.where(mine, t, owner)
    place = key - reqs * length
    owner = jnp.where((place >= 0) & (place < reqs), place, owner)
    row = lax.rem(lax.broadcasted_iota(jnp.int32, (rows, held), 0), reqs)
    valid = row == owner
    states = []
    for k in range(KVH):
        s = scores_of(queries[k], kv_all[0:held, k * HD : (k + 1) * HD])
        s = jnp.where(valid, s, NEG)
        top = jnp.max(s, 1, keepdims=True)
        e = jnp.exp(s - top)
        total = jnp.sum(e, 1, keepdims=True)
        mixed = jnp.dot(
            e.astype(jnp.bfloat16),
            kv_all[0:held, half + k * HD : half + (k + 1) * HD],
            preferred_element_type=jnp.float32,
        )
        states.append((top, total, mixed))
    return states


def heads_aside(mixed, reqs):
    sub8 = lax.broadcasted_iota(jnp.int32, (8, HD), 0)
    parts = []
    for piece_of in mixed:
        for i in range(QH // KVH // 2):
            piece = piece_of[8 * i : 8 * i + 8]
            turned = pltpu.roll(piece, reqs, 0)
            parts.append(jnp.where(sub8 < reqs, piece, turned))
            parts.append(jnp.where(sub8 < reqs, turned, piece))
    return jnp.concatenate(parts, 1)


def attend_window(counts_ref, queries, states, kv_all, me, reqs, span, held, values_here):
    half = KVH * HD
    rows = queries[0].shape[0]
    counts = counts_ref[...]
    lane = lax.broadcasted_iota(jnp.int32, counts.shape, 1)
    offset = jnp.sum(jnp.where(lane < me, counts, 0), 1, keepdims=True)
    taken = jnp.sum(jnp.where(lane == me, counts, 0), 1, keepdims=True)
    first = offset * BLOCK - me * span
    stop = first + taken * BLOCK
    place = lax.broadcasted_iota(jnp.int32, (rows, 2 * span), 1)
    row = lax.rem(lax.broadcasted_iota(jnp.int32, (rows, 2 * span), 0), reqs)
    live = (row == 0) & (place >= first) & (place < stop)
    weights = []
    for k in range(KVH):
        top, total, mixed = states[k]
        s = scores_of(queries[k], kv_all[held : held + 2 * span, k * HD : (k + 1) * HD])
        s = jnp.where(live, s, NEG)
        new = jnp.maximum(top, jnp.max(s, 1, keepdims=True))
        fade = jnp.exp(top - new)
        e = jnp.exp(s - new)
        total = total * fade + jnp.sum(e, 1, keepdims=True)
        weights.append((e.astype(jnp.bfloat16), mixed * fade, total))
    values_here()
    parts = []
    for k in range(KVH):
        e, mixed, total = weights[k]
        mixed = mixed + jnp.dot(
            e,
            kv_all[held : held + 2 * span, half + k * HD : half + (k + 1) * HD],
            preferred_element_type=jnp.float32,
        )
        parts.append(mixed / total)
    return heads_aside(parts, reqs)


def layer_kernel(
    lens_hbm, ids_hbm, route_hbm, tokens_hbm, queries_hbm, own_hbm, counts_hbm, gain_hbm,
    cache_hbm, fresh_hbm, gate_hbm, up_hbm, down_hbm, out_ref,
    lens_ref, ids_ref, route_ref, tokens_ref, queries_ref, own_ref, counts_ref, gain_ref,
    query8, token8, own8, hidden8, kv_all, coef_row, perm_ref, back_ref,
    gathered, coefs, coef_cols, wide, sums, act, part, crossed, hops, fin, w_in, w_down,
    sem_w, sem_kv, sem_in, win_send, win_recv, c_send, c_recv, p_send, p_recv, g_send, g_recv, gx_send, gx_recv,
    x_send, x_recv, r_send, r_recv, f_send, f_recv,
):
    n = lax.axis_size("dev_0")
    half_n = n // 2
    core = lax.axis_index("dev_2")
    other = 1 - core
    sgn = 1 - 2 * core
    xy = {"dev_0": lax.axis_index("dev_0"), "dev_1": lax.axis_index("dev_1")}
    pos = [xy[a] for a in RING]
    line = [xy[a] for a in LINE]
    width = gathered.shape[6]
    reqs = tokens_hbm.shape[0]
    length = cache_hbm.shape[1]
    span = fresh_hbm.shape[0]
    devices = 2 * n * n
    held = reqs * length + 128
    me = (xy["dev_0"] * n + xy["dev_1"]) * 2 + core

    def wrap(v):
        return lax.rem(v + 2 * n, n)

    def place_of(index):
        index = lax.rem(index + devices, devices)
        return {"dev_0": index // (2 * n), "dev_1": lax.rem(index // 2, n), "dev_2": lax.rem(index, 2)}

    barrier = pltpu.get_barrier_semaphore()
    for step in (-1, 1):
        pl.semaphore_signal(barrier, inc=1, device_id=place_of(me + step), device_id_type=MESH_ID)
    pl.semaphore_signal(barrier, inc=1, device_id={"dev_2": other}, device_id_type=MESH_ID)
    for axis in LINE:
        for j in range(1, n):
            pl.semaphore_signal(
                barrier, inc=1, device_id={axis: wrap(xy[axis] + j)}, device_id_type=MESH_ID
            )
    kv_loads = [
        pltpu.make_async_copy(cache_hbm.at[t], kv_all.at[pl.ds(t * length, length)], sem_kv.at[t])
        for t in range(reqs)
    ]
    kv_loads.append(
        pltpu.make_async_copy(fresh_hbm, kv_all.at[pl.ds(held, span)], sem_kv.at[reqs])
    )
    small = (
        (queries_hbm, queries_ref), (tokens_hbm, tokens_ref), (own_hbm, own_ref), (lens_hbm, lens_ref),
        (ids_hbm, ids_ref), (route_hbm, route_ref), (counts_hbm, counts_ref), (gain_hbm, gain_ref),
    )
    small_loads = [
        pltpu.make_async_copy(src, dst, sem_in.at[i]) for i, (src, dst) in enumerate(small)
    ]
    for load in small_loads + kv_loads:
        load.start()
    quarter = 2 * width
    units = gate_hbm.shape[1]
    loads = []
    for h in range(2):
        for q in range(4):
            for k, src in enumerate((gate_hbm, up_hbm)):
                loads.append(
                    pltpu.make_async_copy(
                        src.at[pl.ds(q * quarter + h * width, width)],
                        w_in.at[h, pl.ds(q * width, width), pl.ds(k * units, units)],
                        sem_w.at[(h * 4 + q) * 2 + k],
                    )
                )
    loads.append(pltpu.make_async_copy(down_hbm, w_down, sem_w.at[16]))
    for load in loads:
        load.start()

    for load in small_loads:
        load.wait()
    query = queries_ref[...].astype(jnp.float32)
    query8[0:reqs] = query
    query8[reqs : 2 * reqs] = query
    token = tokens_ref[...].astype(jnp.float32)
    token8[0:reqs] = token
    token8[reqs : 2 * reqs] = token
    own8[...] = jnp.zeros_like(own8)
    own8[0:reqs] = own_ref[...].astype(jnp.float32)
    kv_all[pl.ds(reqs * length, 16)] = own8[...].astype(jnp.bfloat16)
    kv_all[pl.ds(reqs * length + 16, 112)] = jnp.zeros((112, kv_all.shape[1]), jnp.bfloat16)
    lane = lax.broadcasted_iota(jnp.int32, (1, 128), 1)
    coef = jnp.zeros((1, 128), jnp.float32)
    for t in range(reqs):
        for k in range(2):
            coef = coef + jnp.where(lane == t * EXPERTS + ids_ref[k : k + 1, t : t + 1], route_ref[k : k + 1, t : t + 1], 0.0)
    coef_row[...] = coef
    kv_loads[reqs].wait()
    pl.semaphore_wait(barrier, 2 * (n - 1) + 3)

    pending = []

    def send(src, dst, s_sem, r_sem, where):
        copy = pltpu.make_async_remote_copy(
            src_ref=src, dst_ref=dst, send_sem=s_sem, recv_sem=r_sem,
            device_id=where, device_id_type=MESH_ID,
        )
        copy.start()
        pending.append(copy)
        return copy

    columns = KVH * HD
    following = [
        send(
            kv_all.at[pl.ds(held, span), pl.ds(i * columns, columns)],
            kv_all.at[pl.ds(held + span, span), pl.ds(i * columns, columns)],
            win_send.at[i], win_recv.at[i], place_of(me - 1),
        )
        for i in range(2)
    ]
    static_slot = {o % n: i for i, o in enumerate(OFFSETS)}
    coefs[core, 0, 0] = coef_row[...]
    coef_firsts = [
        send(
            coef_row, coefs.at[core, 0, static_slot[-j % n]], c_send.at[j], c_recv.at[j],
            {"dev_0": wrap(xy["dev_0"] + j)},
        )
        for j in range(1, n)
    ]
    size = perm_ref.shape[0]

    def parts_of(r):
        return r // (size // 4), lax.rem(r // (2 * reqs), n), lax.rem(r // reqs, 2), lax.rem(r, reqs)

    def stacked_row(r):
        q, b, c, t = parts_of(r)
        return c * (size // 2) + b * 16 + q * reqs + t

    def waved_row(r):
        q, b, c, t = parts_of(r)
        wave = 1 - t // 2
        return wave * (size // 2) + c * (size // 4) + b * 8 + lax.rem(t, 2) * 4 + q

    row = lax.broadcasted_iota(jnp.int32, (size, 1), 0)
    column = lax.broadcasted_iota(jnp.int32, (1, size), 1)
    perm_ref[...] = (waved_row(row) == column).astype(jnp.float32).astype(jnp.bfloat16)
    back_ref[...] = (row == stacked_row(column)).astype(jnp.float32).astype(jnp.bfloat16)
    for load in kv_loads[:reqs]:
        load.wait()
    queries = query_rows(query8, reqs)
    states = attend_held(lens_ref, queries, kv_all, reqs, length, held)
    token = token8[...]
    gain = gain_ref[...]
    row8 = lax.broadcasted_iota(jnp.int32, (8, quarter), 0)

    def normed_of(hidden):
        mean = jnp.mean(hidden * hidden, 1, keepdims=True)
        return hidden * lax.rsqrt(mean + EPS) * gain

    def put(wave, normed):
        block = jnp.zeros((8, quarter), jnp.float32)
        for i in range(2):
            t = 2 * (1 - wave) + i
            for q in range(4):
                line_of = jnp.broadcast_to(
                    normed[t : t + 1, q * quarter : (q + 1) * quarter], (8, quarter)
                )
                block = jnp.where(row8 == i * 4 + q, line_of, block)
        block = block.astype(jnp.bfloat16)
        for h in range(2):
            gathered[wave, h, core, 0, 0] = block[:, h * width : (h + 1) * width]

    passing = {}

    def depart(wave):
        for slot in range(1, n) if wave == 0 else range(n - 1, 0, -1):
            for h in range(2):
                offset = OFFSETS[slot]
                passing[wave, h, slot] = send(
                    gathered.at[wave, h, core, 0, 0],
                    gathered.at[wave, h, core, 0, static_slot[-offset % n]],
                    p_send.at[wave, h, slot], p_recv.at[wave, h, slot],
                    {LINE[h]: wrap(line[h] + offset)},
                )

    early = heads_aside([mixed / total for _, total, mixed in states], reqs)
    put(0, normed_of(token + early))
    depart(0)
    following[0].wait_recv()
    hidden = token + attend_window(
        counts_ref, queries, states, kv_all, me, reqs, span, held, following[1].wait_recv
    )
    hidden8[...] = hidden
    put(1, normed_of(hidden))
    depart(1)

    ways = ((0, half_n, sgn), (1, half_n - 1, -sgn))
    def arrive(wave, g):
        low, count = NEAR_AND_FAR[g]
        for slot in range(max(low, 1), low + count):
            for h in range(2):
                passing[wave, h, slot].wait_recv()

    rounds = {}
    crossing = {}

    def go_round(wave, s, g):
        low, count = NEAR_AND_FAR[g]
        at = pl.ds(low, count)
        for h in range(2):
            for way, steps, turn in ways:
                if s > 1 and s - 1 <= steps:
                    rounds[wave, h, way, s - 1, g].wait_recv()
                if s <= steps:
                    rounds[wave, h, way, s, g] = send(
                        gathered.at[wave, h, core, slot_at(-turn, s - 1), at],
                        gathered.at[wave, h, core, slot_at(-turn, s), at],
                        g_send.at[wave, h, way, s - 1, g], g_recv.at[wave, h, way, s - 1, g],
                        {RING[h]: wrap(pos[h] + turn)},
                    )
        for h in range(2):
            first, many = slots_of(s - 1)
            ref = gathered.at[wave, h, core, pl.ds(first, many), at]
            crossing[wave, h, s - 1, g] = send(
                ref, ref, gx_send.at[wave, h, s - 1, g], gx_recv.at[wave, h, s - 1, g],
                {"dev_2": other},
            )

    batch = 2 * n * reqs
    stack = 4 * batch

    def project(d):
        if d == 0:
            for load in loads[:16]:
                load.wait()
        first, many = slots_of(d)
        for h in range(2):
            for wave in range(2):
                for g in range(len(NEAR_AND_FAR)):
                    crossing[wave, h, d, g].wait_recv()
            for i in range(many):
                z = gathered[:, h, :, first + i].reshape(stack, width)
                z = jnp.dot(perm_ref[...], z, preferred_element_type=jnp.float32).astype(jnp.bfloat16)
                for q in range(4):
                    wide[i * batch : (i + 1) * batch, q * width : (q + 1) * width] = z[
                        q * batch : (q + 1) * batch
                    ]
            sums[h, first * batch : (first + many) * batch] = jnp.dot(
                wide[0 : many * batch], w_in[h], preferred_element_type=jnp.float32
            )

    arrive(0, 0)
    go_round(0, 1, 0)
    arrive(0, 1)
    go_round(0, 1, 1)
    for copy in coef_firsts:
        copy.wait_recv()
    coef_seconds = [
        send(
            coefs.at[core, 0], coefs.at[core, static_slot[-j % n]],
            c_send.at[n + j], c_recv.at[n + j], {"dev_1": wrap(xy["dev_1"] + j)},
        )
        for j in range(1, n)
    ]
    go_round(0, 2, 0)
    go_round(0, 2, 1)
    arrive(1, 1)
    go_round(1, 1, 1)
    arrive(1, 0)
    go_round(1, 1, 0)
    go_round(0, 3, 0)
    go_round(0, 3, 1)
    go_round(1, 2, 1)
    go_round(1, 2, 0)
    project(0)
    go_round(0, 4, 0)
    go_round(0, 4, 1)
    go_round(1, 3, 1)
    go_round(1, 3, 0)
    project(1)
    for copy in coef_seconds:
        copy.wait_recv()
    coef_both = send(coefs.at[core], coefs.at[core], c_send.at[0], c_recv.at[0], {"dev_2": other})
    go_round(0, 5, 0)
    go_round(0, 5, 1)
    go_round(1, 4, 1)
    go_round(1, 4, 0)
    project(2)
    coef_both.wait_recv()
    expert = me // (devices // EXPERTS)
    row8 = lax.broadcasted_iota(jnp.int32, (8, 128), 0)
    lane8 = lax.broadcasted_iota(jnp.int32, (8, 128), 1)
    keep = lane8 == lax.rem(row8, reqs) * EXPERTS + expert
    for r in range(n):
        for c in range(n):
            both = jnp.where(row8 < reqs, coefs[0, r, c], coefs[1, r, c])
            coef_cols[r, c] = jnp.broadcast_to(
                jnp.sum(jnp.where(keep, both, 0.0), 1, keepdims=True), (8, 128)
            )
    go_round(1, 5, 1)
    project(3)
    go_round(1, 5, 0)
    project(4)

    for r in range(n):
        both = sums[0, r * batch : (r + 1) * batch] + jnp.concatenate(
            [sums[1, c * batch + r * 8 : c * batch + (r + 1) * 8] for c in range(n)], 0
        )
        gate = both[:, :units]
        up = both[:, units:]
        coef = coef_cols[r].reshape(batch, 128)
        coef = jnp.concatenate([coef] * (units // 128), 1)
        act[r] = (gate / (1.0 + jnp.exp(-gate)) * up * coef).reshape(n, 8, units)
    loads[16].wait()

    crossed_copies = {}

    def descend(d):
        first, many = slots_of(d)
        for h in range(2):
            if h == 0:
                rows = [act[first + i].reshape(batch, units) for i in range(many)]
            else:
                rows = [act[:, first + i].reshape(batch, units) for i in range(many)]
            a = jnp.concatenate(rows, 0).astype(jnp.bfloat16)
            for q in range(4):
                wide[0 : many * batch, q * width : (q + 1) * width] = jnp.dot(
                    a,
                    w_down[:, q * quarter + h * width : q * quarter + (h + 1) * width],
                    preferred_element_type=jnp.float32,
                ).astype(jnp.bfloat16)
            for i in range(many):
                z = jnp.concatenate(
                    [
                        wide[i * batch : (i + 1) * batch, q * width : (q + 1) * width]
                        for q in range(4)
                    ],
                    0,
                )
                z = jnp.dot(back_ref[...], z, preferred_element_type=jnp.float32)
                part[h, :, first + i] = z.astype(jnp.bfloat16).reshape(2, n, 16, width)
            at = pl.ds(first, many)
            crossed_copies[h, d] = send(
                part.at[h, other, at], crossed.at[h, at], x_send.at[h, d], x_recv.at[h, d],
                {"dev_2": other},
            )

    holding = {}

    def collect(k):
        distance = half_n + 1 - k
        for h in range(2):
            crossed_copies[h, distance].wait_recv()
        for g in (2, 1, 0):
            low, count = GROUPS_OF_BLOCKS[g]
            at = pl.ds(low, count)
            for h in range(2):
                for way, steps, turn in ways:
                    s = k - (half_n - steps)
                    if s < 1:
                        continue
                    slot = slot_at(turn, distance)
                    total = part[h, core, slot, at].astype(jnp.float32) + crossed[h, slot, at].astype(
                        jnp.float32
                    )
                    if s > 1:
                        holding[h, way, s - 1, g].wait_recv()
                        total = total + hops[h, way, s - 2, at].astype(jnp.float32)
                    part[h, core, slot, at] = total.astype(jnp.bfloat16)
                    holding[h, way, s, g] = send(
                        part.at[h, core, slot, at], hops.at[h, way, s - 1, at],
                        r_send.at[h, way, s - 1, g], r_recv.at[h, way, s - 1, g],
                        {RING[h]: wrap(pos[h] + turn)},
                    )

    def collect_own(g):
        low, count = GROUPS_OF_BLOCKS[g]
        at = pl.ds(low, count)
        for h in range(2):
            total = part[h, core, 0, at].astype(jnp.float32) + crossed[h, 0, at].astype(jnp.float32)
            for way, steps, turn in ways:
                holding[h, way, steps, g].wait_recv()
                total = total + hops[h, way, steps - 1, at].astype(jnp.float32)
            part[h, core, 0, at] = total.astype(jnp.bfloat16)
        for slot in reversed(range(max(low, 1), low + count)):
            for h in range(2):
                finals.append(
                    send(
                        part.at[h, core, 0, slot], fin.at[h, slot], f_send.at[h, slot], f_recv.at[h, slot],
                        {LINE[h]: wrap(line[h] + OFFSETS[slot])},
                    )
                )

    finals = []
    descend(4)
    descend(3)
    collect(1)
    descend(2)
    collect(2)
    descend(1)
    collect(3)
    descend(0)
    collect(4)
    for h in range(2):
        crossed_copies[h, 0].wait_recv()
    collect_own(2)
    collect_own(1)
    collect_own(0)
    for copy in finals:
        copy.wait_recv()
    totals = []
    for h in range(2):
        total = part[h, core, 0, 0].astype(jnp.float32)
        for slot in range(1, n):
            total = total + fin[h, slot].astype(jnp.float32)
        totals.append(total)
    moe = jnp.concatenate(totals, 1)
    pieces = []
    for i in range(2):
        pieces.append(moe[8 * i : 8 * i + 8])
        pieces.append(pltpu.roll(moe[8 * i : 8 * i + 8], reqs, 0))
    final = hidden8[...] + jnp.concatenate(pieces, 1)
    out_ref[...] = final[0:reqs]
    for copy in pending:
        copy.wait_send()


def per_device(
    tokens,
    queries,
    token_kv,
    kv_cache,
    context_lengths,
    fresh_kv,
    block_counts,
    expert_ids,
    route_weights,
    norm_gain,
    w_gate,
    w_up,
    w_down,
):
    n = lax.axis_size("dev_0")
    reqs, full = tokens.shape
    width = full // 8
    units = w_gate.shape[1]
    rows = 2 * n * n * reqs
    size = 4 * 2 * n * reqs
    vmem = pl.BlockSpec(memory_space=pltpu.VMEM)
    anyspace = pl.BlockSpec(memory_space=pl.ANY)
    bf = jnp.bfloat16
    f32 = jnp.float32
    dma = pltpu.SemaphoreType.DMA
    half_n = n // 2
    keys = reqs * kv_cache.shape[1] + 2 * fresh_kv.shape[0] + 128
    result = pl.pallas_call(
        layer_kernel,
        out_shape=jax.ShapeDtypeStruct(tokens.shape, f32),
        in_specs=[anyspace] * 13,
        out_specs=vmem,
        scratch_shapes=[
            pltpu.VMEM((1, reqs), jnp.int32),
            pltpu.VMEM((2, reqs), jnp.int32),
            pltpu.VMEM((2, reqs), f32),
            pltpu.VMEM(tokens.shape, bf),
            pltpu.VMEM(queries.shape, bf),
            pltpu.VMEM(token_kv.shape, bf),
            pltpu.VMEM((1, block_counts.shape[0]), jnp.int32),
            pltpu.VMEM((1, full), f32),
            pltpu.VMEM((2 * reqs, full), f32),
            pltpu.VMEM((2 * reqs, full), f32),
            pltpu.VMEM((16, token_kv.shape[1]), f32),
            pltpu.VMEM((2 * reqs, full), f32),
            pltpu.VMEM((keys, token_kv.shape[1]), bf),
            pltpu.VMEM((1, 128), f32),
            pltpu.VMEM((size, size), bf),
            pltpu.VMEM((size, size), bf),
            pltpu.VMEM((2, 2, 2, n, n, 8, width), bf),
            pltpu.VMEM((2, n, n, 1, 128), f32),
            pltpu.VMEM((n, n, 8, 128), f32),
            pltpu.VMEM((4 * n * reqs, full // 2), bf),
            pltpu.VMEM((2, rows, 2 * units), f32),
            pltpu.VMEM((n, n, 8, units), f32),
            pltpu.VMEM((2, 2, n, n, 16, width), bf),
            pltpu.VMEM((2, n, n, 16, width), bf),
            pltpu.VMEM((2, 2, half_n, n, 16, width), bf),
            pltpu.VMEM((2, n, 16, width), bf),
            pltpu.VMEM((2, full // 2, 2 * units), bf),
            pltpu.VMEM(w_down.shape, bf),
            dma((17,)),
            dma((reqs + 1,)),
            dma((8,)),
            dma((2,)), dma((2,)),
            dma((2 * n,)), dma((2 * n,)),
            dma((2, 2, n)), dma((2, 2, n)),
            dma((2, 2, 2, half_n, 2)), dma((2, 2, 2, half_n, 2)),
            dma((2, 2, half_n + 1, 2)), dma((2, 2, half_n + 1, 2)),
            dma((2, half_n + 1)), dma((2, half_n + 1)),
            dma((2, 2, half_n, 3)), dma((2, 2, half_n, 3)),
            dma((2, n)), dma((2, n)),
        ],
        compiler_params=pltpu.CompilerParams(
            collective_id=0, has_side_effects=True, vmem_limit_bytes=60 * 1024 * 1024
        ),
    )(
        context_lengths.reshape(1, -1), expert_ids.T, route_weights.T, tokens, queries, token_kv,
        block_counts.reshape(1, -1), norm_gain.reshape(1, -1),
        kv_cache, fresh_kv, w_gate, w_up, w_down,
    )
    return result.astype(bf)


def solution(mesh):
    split = Mesh(
        mesh.devices.reshape(mesh.shape["groups"], 8, 8, 2), ("groups", "dev_0", "dev_1", "dev_2")
    )
    return jax.shard_map(
        per_device,
        mesh=split,
        in_specs=(
            P(GROUPS_DEV, None),
            P(GROUPS_DEV, None),
            P(GROUPS_DEV, None),
            P(GROUPS_DEV, None, None),
            P(GROUPS_DEV),
            P(GROUPS_DEV, None),
            P("groups"),
            P(GROUPS_DEV, None),
            P(GROUPS_DEV, None),
            P(),
            P(None, DEV),
            P(None, DEV),
            P(DEV, None),
        ),
        out_specs=P(GROUPS_DEV, None),
        check_vma=False,
    )
```
